256 devices in a mesh: pa: 16 (over x_hi, z), gz: 16 (over x_lo, y, core).
Axes of the slice: x: 4 (x_hi: 2, x_lo: 2; x = x_hi * 2 + x_lo), y: 4, z: 8, core: 2. Of those that a mesh axis runs over, the one named last changes fastest.
Arguments:
- source: float32 [128, 768, 768], P('gz', 'pa'), may hold values from -24 to 24
- cell_width: float32 [128], P('gz'), may hold values from 0.5 to 2
Outputs:
- potential: float32 [128, 768, 768], P('gz', 'pa')
The draws below stay inside these ranges and needn't reach their ends.
All inputs are finite; a program needn't handle non-finite values.
Results may differ from the reference program's by a relative error of at most 0.00085.
Values sent between devices are 32-bit elements; how exact they have to be, the bound alone decides.
No kernel may reach another device: no remote copies, remote signals or barrier semaphores. Data moves between devices by JAX's collectives and lax.ppermute only.
A program may use at most 64 MiB of HBM per device.

```python
import math
import jax
import jax.numpy as jnp
from jax import lax

NX = 768
NY = 768
NZ = 128


def laplace_field(field):
    mirrored = jnp.concatenate([field[:, :, :1], field, field[:, :, -1:]], 2)
    across = 2.0 * field - mirrored[:, :, :-2] - mirrored[:, :, 2:]
    padded_rows = jnp.pad(field, ((0, 0), (1, 1), (0, 0)))
    columns = 2.0 * field - padded_rows[:, :-2, :] - padded_rows[:, 2:, :]
    padded_depth = jnp.pad(field, ((1, 1), (0, 0), (0, 0)))
    along_depth = 2.0 * field - padded_depth[:-2] - padded_depth[2:]
    return across + columns + along_depth


def draw_source(key, part):
    rough = jnp.clip(jax.random.normal(key, (NZ, NY, NX), jnp.float32), -4.0, 4.0)
    return 0.5 * laplace_field(rough)


def shard_levels(stream_key, shape, shards, smallest, top_value):
    gain, own = 1.0, jax.random.fold_in(stream_key, 6)
    for dim, shards_of in shards:
        heights = jnp.exp(jax.random.uniform(jax.random.fold_in(own, dim), (shards_of,), jnp.float32, smallest / len(shards), top_value / len(shards)))
        gain = gain * jnp.repeat(heights, shape[dim] // shards_of).reshape([-1 if axis == dim else 1 for axis in range(len(shape))])
    return gain


def setup_inputs(seed: int = 0) -> dict:
    splits = jax.random.split(jax.random.key(seed), 3)
    return {
        "source": draw_source(jax.random.fold_in(splits[2], 71), 0),
        "cell_width": jnp.clip(jnp.exp(math.log(2.0) - 1.3862944 * jax.random.uniform(splits[1], (NZ,), jnp.float32) ** shard_levels(splits[1], (NZ,), ((0, 16),), -0.2, 0.2)), 0.5, 2.0),
    }


HIGHEST = lax.Precision.HIGHEST

def cosine_table(width):
    counter = jnp.arange(width, dtype=jnp.int32)
    phases = counter[:, None] * (2 * counter[None, :] + 1) % (4 * width)
    angles = phases.astype(jnp.float32) * (math.pi / (2 * width))
    weights = jnp.where(counter == 0, math.sqrt(1.0 / width), math.sqrt(2.0 / width)).astype(jnp.float32)
    return weights[:, None] * jnp.cos(angles)

def sine_table(width):
    counter = jnp.arange(1, width + 1, dtype=jnp.int32)
    phases = counter[:, None] * counter[None, :] % (2 * (width + 1))
    angles = phases.astype(jnp.float32) * (math.pi / (width + 1))
    return math.sqrt(2.0 / (width + 1)) * jnp.sin(angles)

def eigen_first(offset, count, width):
    wavenumber = (offset + jnp.arange(count, dtype=jnp.int32)).astype(jnp.float32)
    return 4.0 * jnp.square(jnp.sin(wavenumber * (math.pi / (2 * width))))

def eigen_second(width):
    wavenumber = jnp.arange(1, width + 1, dtype=jnp.int32).astype(jnp.float32)
    return 4.0 * jnp.square(jnp.sin(wavenumber * (math.pi / (2 * (width + 1)))))

def reference(source, cell_width):
    cos_table = cosine_table(NX)
    sin_table = sine_table(NY)
    padded = jnp.pad(cell_width, 1)
    upper_coef = 2.0 / (padded[1:-1] + padded[2:])
    lower_coef = 2.0 / (padded[:-2] + padded[1:-1])
    along_x = jnp.einsum('zyi,ki->zky', source, cos_table, precision=HIGHEST)
    spectral = jnp.einsum('zkj,lj->zkl', along_x, sin_table, precision=HIGHEST)
    eigen_sum = eigen_first(0, NX, NX)[:, None] + eigen_second(NY)[None, :]

    def eliminate(previous, entries):
        below_coef, above_coef, width_cell, forcing = entries
        diagonal = below_coef + above_coef + width_cell * eigen_sum
        divisor = diagonal + below_coef * previous[0]
        ratio_now = -above_coef / divisor
        value_now = (width_cell * forcing + below_coef * previous[1]) / divisor
        return ((ratio_now, value_now), (ratio_now, value_now))
    zero_plane = jnp.zeros((NX, NY), jnp.float32)
    _, (ratios, values) = lax.scan(eliminate, (zero_plane, zero_plane), (lower_coef, upper_coef, cell_width, spectral))

    def substitute(following, entries):
        current = entries[1] - entries[0] * following
        return (current, current)
    _, solved = lax.scan(substitute, zero_plane, (ratios, values), reverse=True)
    along_y = jnp.einsum('zkl,lj->zkj', solved, sin_table, precision=HIGHEST)
    return jnp.einsum('zky,ki->zyi', along_y, cos_table, precision=HIGHEST)
```

```python
import functools
import math

import numpy as np

import jax
import jax.numpy as jnp
from jax import lax
from jax.experimental import pallas as pl
from jax.experimental.pallas import tpu as pltpu
from jax.sharding import Mesh
from jax.sharding import PartitionSpec as P

GZ = ("gz_0", "gz_1", "gz_2")
LANES = 128
VMEM = pltpu.MemorySpace.VMEM
SMEM = pltpu.MemorySpace.SMEM


def halves(table):
    table = table.astype(np.float32)
    high = table.astype(jnp.bfloat16)
    low = (table - high.astype(np.float32)).astype(jnp.bfloat16)
    return high, low


def cosine_rows(width):
    k = np.arange(width)
    phases = k[:, None] * (2 * k[None, :] + 1) % (4 * width)
    weights = np.where(k == 0, math.sqrt(1.0 / width), math.sqrt(2.0 / width))
    return weights[:, None] * np.cos(phases * (math.pi / (2 * width)))


def sine_rows(width):
    k = np.arange(1, width + 1)
    phases = k[:, None] * k[None, :] % (2 * (width + 1))
    return math.sqrt(2.0 / (width + 1)) * np.sin(phases * (math.pi / (width + 1)))


def eigen_first(offset, count, width):
    wavenumber = (offset + jnp.arange(count, dtype=jnp.int32)).astype(jnp.float32)
    return 4.0 * jnp.square(jnp.sin(wavenumber * (math.pi / (2 * width))))


def eigen_second(width):
    wavenumber = jnp.arange(1, width + 1, dtype=jnp.int32).astype(jnp.float32)
    return 4.0 * jnp.square(jnp.sin(wavenumber * (math.pi / (2 * (width + 1)))))


def split(x):
    high = x.astype(jnp.bfloat16)
    return high, (x - high.astype(jnp.float32)).astype(jnp.bfloat16)


def dot3(x, t_high, t_low, dims):
    high, low = split(x)
    dot = functools.partial(
        lax.dot_general, dimension_numbers=(dims, ((), ())), preferred_element_type=jnp.float32
    )
    return dot(high, t_high) + dot(low, t_high) + dot(high, t_low)


def swap_groups(blocks, group):
    n = len(blocks)
    lanes = n * group
    lane = lax.broadcasted_iota(jnp.int32, blocks[0].shape, 1)
    blocks = list(blocks)
    d = 1
    while d < n:
        keep = (lane & (d * group)) == 0
        for i in range(n):
            if i & d:
                continue
            a, b = blocks[i], blocks[i + d]
            blocks[i] = jnp.where(keep, a, pltpu.roll(b, d * group, 1))
            blocks[i + d] = jnp.where(keep, pltpu.roll(a, lanes - d * group, 1), b)
        d *= 2
    return blocks


def forward_x(src_ref, ch_ref, cl_ref, out_ref, acc_ref, *, depth, rows, peers, group):
    acc_ref[...] = dot3(src_ref[...], ch_ref[...], cl_ref[...], ((1,), (1,)))
    for c in range(peers // depth):
        lanes = pl.ds(c * LANES, LANES)
        blocks = [acc_ref[pl.ds(z * rows, rows), lanes] for z in range(depth)]
        for g, block in enumerate(swap_groups(blocks, group)):
            out_ref[c * depth + g] = block


def backward_x(*refs, depth, rows, peers, group):
    chunks = (len(refs) - 2) // 3
    out_ref, x_ref = refs[-2], refs[-1]
    for m in range(chunks):
        msg_ref, ch_ref, cl_ref = refs[3 * m : 3 * m + 3]
        for c in range(peers // depth):
            blocks = [msg_ref[c * depth + g] for g in range(depth)]
            for z, block in enumerate(swap_groups(blocks, group)):
                x_ref[pl.ds(z * rows, rows), pl.ds(c * LANES, LANES)] = block
        part = dot3(x_ref[...], ch_ref[...], cl_ref[...], ((1,), (0,)))
        if m == 0:
            out_ref[...] = part
        else:
            out_ref[...] += part


def sweep(lower, upper, width, eigen, depth, forcing=None):
    left, right, value = [None], [None], [None]
    for i in range(1, depth):
        diagonal = (lower(i) + upper(i)) + width(i) * eigen
        if i == 1:
            inverse = 1.0 / diagonal
            left.append(-(inverse * lower(i)))
        else:
            inverse = 1.0 / (diagonal + lower(i) * right[-1])
            left.append(inverse * lower(i) * left[-1])
        if forcing is not None:
            f = width(i) * forcing(i)
            value.append(inverse * (f if i == 1 else f + lower(i) * value[-1]))
        right.append(-(inverse * upper(i)))
    return left, right, value


def head_inverse(lower, upper, width, eigen, left, right, depth):
    inner_left, inner_right = left[depth - 2], right[depth - 2]
    for i in range(depth - 3, 0, -1):
        inner_left = left[i] - right[i] * inner_left
        inner_right = -(right[i] * inner_right)
    diagonal = (lower(0) + upper(0)) + width(0) * eigen
    return 1.0 / (diagonal + upper(0) * inner_left), inner_right


def reader(ref, offset=0):
    return lambda i: ref[offset + i]


def middle_forward(
    low_ref, up_ref, wid_ref, msg_ref, sh_ref, sl_ref, ek_ref, el_ref, val_ref, bnd_ref, acc_ref,
    *, depth, group, tile
):
    lower, upper, width = reader(low_ref), reader(up_ref), reader(wid_ref)
    rows = msg_ref.shape[0] * msg_ref.shape[1]
    x = msg_ref[...].reshape(rows, LANES).T
    acc_ref[...] = dot3(x, sh_ref[...], sl_ref[...], ((1,), (0,)))
    bnd_ref[...] = jnp.zeros(bnd_ref.shape, jnp.float32)
    wide = el_ref.shape[1]
    half = group
    for t in range(wide // tile):
        cols = pl.ds(t * tile, tile)
        eigen = ek_ref[...] + el_ref[:, cols]
        forcing = lambda i: acc_ref[pl.ds(i * group, group), cols]
        left, right, value = sweep(lower, upper, width, eigen, depth, forcing)
        inverse, _ = head_inverse(lower, upper, width, eigen, left, right, depth)
        inner = value[depth - 2]
        for i in range(depth - 3, 0, -1):
            inner = value[i] - right[i] * inner
        head = inverse * (width(0) * forcing(0) + upper(0) * inner)
        tail = value[depth - 1]
        for i in range(1, depth - 1):
            val_ref[i - 1, :, cols] = value[i]
        for s in range(group // 8):
            for c in range(tile // LANES):
                part = (slice(s * 8, s * 8 + 8), slice(c * LANES, c * LANES + LANES))
                start = s * 8 * half + t * (tile // LANES) + c
                bnd_ref[pl.ds(start, 8, stride=half), :] = head[part]
                bnd_ref[pl.ds(start + 8, 8, stride=half), :] = tail[part]


def column_solve(low_ref, up_ref, wid_ref, ek_ref, el_ref, *refs, depth, blocks):
    chunks = len(refs) // 2
    for m in range(chunks):
        in_ref, out_ref = refs[m], refs[chunks + m]
        eigen = ek_ref[m] + el_ref[...]
        ratio = rhs = None
        swept = []
        for q in range(blocks):
            lower, upper, width = (reader(r, q * depth) for r in (low_ref, up_ref, wid_ref))
            left, right, _ = sweep(lower, upper, width, eigen, depth)
            inverse, inner_right = head_inverse(lower, upper, width, eigen, left, right, depth)
            below = -(inverse * lower(0))
            above = inverse * upper(0) * inner_right
            tail_below, tail_above = left[depth - 1], right[depth - 1]
            head_in, tail_in = in_ref[q, 0:8, :], in_ref[q, 8:16, :]
            if q == 0:
                head_ratio, head_rhs = above, head_in
            else:
                divided = 1.0 / (1.0 - below * ratio)
                head_ratio = above * divided
                head_rhs = (head_in - below * rhs) * divided
            divided = 1.0 / (1.0 - tail_below * head_ratio)
            ratio = tail_above * divided
            rhs = (tail_in - tail_below * head_rhs) * divided
            swept.append((head_ratio, head_rhs, ratio, rhs))
        following = None
        for q in range(blocks - 1, -1, -1):
            head_ratio, head_rhs, ratio, rhs = swept[q]
            tail = rhs if following is None else rhs - ratio * following
            following = head_rhs - head_ratio * tail
            out_ref[q, 0:8, :] = following
            out_ref[q, 8:16, :] = tail


def middle_backward(
    low_ref, up_ref, wid_ref, bnd_ref, val_ref, sh_ref, sl_ref, ek_ref, el_ref, out_ref, x_ref,
    *, depth, group, tile
):
    lower, upper, width = reader(low_ref), reader(up_ref), reader(wid_ref)
    wide = el_ref.shape[1]
    for s in range(group // 8):
        for c in range(wide // LANES):
            start = s * 8 * group + c
            cols = pl.ds(c * LANES, LANES)
            x_ref[pl.ds(s * 8, 8), cols] = bnd_ref[pl.ds(start, 8, stride=group), :]
            x_ref[pl.ds((depth - 1) * group + s * 8, 8), cols] = bnd_ref[
                pl.ds(start + 8, 8, stride=group), :
            ]
    for t in range(wide // tile):
        cols = pl.ds(t * tile, tile)
        eigen = ek_ref[...] + el_ref[:, cols]
        left, right, _ = sweep(lower, upper, width, eigen, depth - 1)
        head = x_ref[pl.ds(0, group), cols]
        following = x_ref[pl.ds((depth - 1) * group, group), cols]
        for i in range(depth - 2, 0, -1):
            following = val_ref[i - 1, :, cols] - left[i] * head - right[i] * following
            x_ref[pl.ds(i * group, group), cols] = following
    y = dot3(x_ref[...], sh_ref[...], sl_ref[...], ((1,), (0,))).T
    out_ref[...] = y.reshape(out_ref.shape)


def call(kernel, name, out, args, smem=0, scratch=()):
    specs = [pl.BlockSpec(memory_space=SMEM)] * smem
    specs += [pl.BlockSpec(memory_space=VMEM)] * (len(args) - smem)
    outs = jax.tree.map(lambda s: jax.ShapeDtypeStruct(s, jnp.float32), out, is_leaf=lambda s: isinstance(s[0], int))
    return pl.pallas_call(
        kernel,
        name=name,
        out_shape=outs,
        in_specs=specs,
        out_specs=jax.tree.map(lambda s: pl.BlockSpec(memory_space=VMEM), outs),
        scratch_shapes=[pltpu.VMEM(s, jnp.float32) for s in scratch],
    )(*args)


def on_device(source, cell_width):
    depth, rows, width_x = source.shape
    peers = lax.axis_size("pa")
    blocks = lax.axis_size(GZ)
    width_y = rows * peers
    owned = width_x // peers
    group = LANES // depth
    chunks = owned // group
    wide = peers * group

    table = cosine_rows(width_x).reshape(peers, chunks, group, width_x)
    cosines = [
        [jnp.asarray(t) for t in halves(table[:, m].reshape(wide, width_x))] for m in range(chunks)
    ]
    sines = [jnp.asarray(t) for t in halves(sine_rows(width_y))]

    spread = jnp.broadcast_to(cell_width[None, :, None], (blocks, depth, LANES))
    widths = lax.all_to_all(spread, GZ, split_axis=0, concat_axis=0, tiled=True)[:, :, 0].reshape(-1)
    padded = jnp.pad(widths, 1)
    upper = 2.0 / (padded[1:-1] + padded[2:])
    lower = 2.0 / (padded[:-2] + padded[1:-1])
    block = lax.axis_index(GZ)
    own = [lax.dynamic_slice_in_dim(a, block * depth, depth) for a in (lower, upper, widths)]
    eigen_x = eigen_first(lax.axis_index("pa") * owned, owned, width_x).reshape(chunks, group)
    eigen_y = eigen_second(width_y)
    own_x = lax.dynamic_index_in_dim(eigen_x, block, 1, keepdims=False)
    cells_y = jnp.pad(eigen_y.reshape(-1, LANES), ((0, 8 - width_y // LANES), (0, 0)), constant_values=1.0)
    eigen_y = eigen_y[None]

    flat = source.reshape(depth * rows, width_x)
    sizes = dict(depth=depth, rows=rows, peers=peers, group=group)
    values, boundary = [], []
    for m in range(chunks):
        sent = call(
            functools.partial(forward_x, **sizes), f"forward_x_{m}", (peers, rows, LANES),
            (flat, *cosines[m]), scratch=[(depth * rows, wide)],
        )
        got = lax.all_to_all(sent, "pa", split_axis=0, concat_axis=0, tiled=True)
        value, ends = call(
            functools.partial(middle_forward, depth=depth, group=group, tile=width_y // 2),
            f"middle_forward_{m}",
            ((depth - 2, group, width_y), (blocks * group, LANES)),
            (*own, got, *sines, eigen_x[m][:, None], eigen_y),
            smem=3,
            scratch=[(depth * group, width_y)],
        )
        values.append(value)
        ends = ends.reshape(blocks, group, LANES)
        boundary.append(lax.all_to_all(ends, GZ, split_axis=0, concat_axis=0, tiled=True))
    solved = call(
        functools.partial(column_solve, depth=depth, blocks=blocks), "column_solve",
        [(blocks, group, LANES)] * chunks,
        (lower, upper, widths, own_x, cells_y, *boundary), smem=4,
    )
    last = []
    for m in range(chunks):
        ends = lax.all_to_all(solved[m], GZ, split_axis=0, concat_axis=0, tiled=True)
        sent = call(
            functools.partial(middle_backward, depth=depth, group=group, tile=width_y // 2),
            f"middle_backward_{m}",
            (peers, rows, LANES),
            (*own, ends.reshape(blocks * group, LANES), values[m], *sines, eigen_x[m][:, None], eigen_y),
            smem=3,
            scratch=[(depth * group, width_y)],
        )
        last += [lax.all_to_all(sent, "pa", split_axis=0, concat_axis=0, tiled=True), *cosines[m]]
    out = call(
        functools.partial(backward_x, **sizes), "backward_x", (depth * rows, width_x), last,
        scratch=[(depth * rows, wide)],
    )
    return out.reshape(depth, rows, width_x)


def solution(mesh):
    split_mesh = Mesh(mesh.devices.reshape(mesh.shape["pa"], 2, 4, 2), ("pa", "gz_0", "gz_1", "gz_2"))
    return jax.shard_map(
        on_device,
        mesh=split_mesh,
        in_specs=(P(GZ, "pa", None), P(GZ)),
        out_specs=P(GZ, "pa", None),
        check_vma=False,
    )
```

```python
import functools
import math

import numpy as np

import jax
import jax.numpy as jnp
from jax import lax
from jax.experimental import pallas as pl
from jax.experimental.pallas import tpu as pltpu
from jax.sharding import PartitionSpec as P

ALL = ("pa", "gz")
LANES = 128
SUB = 8
VMEM = pltpu.MemorySpace.VMEM


def halves(table):
    table = table.astype(np.float32)
    high = table.astype(jnp.bfloat16)
    low = (table - high.astype(np.float32)).astype(jnp.bfloat16)
    return jnp.asarray(high), jnp.asarray(low)


def cosine_rows(width):
    k = np.arange(width)
    phases = k[:, None] * (2 * k[None, :] + 1) % (4 * width)
    weights = np.where(k == 0, math.sqrt(1.0 / width), math.sqrt(2.0 / width))
    return weights[:, None] * np.cos(phases * (math.pi / (2 * width)))


def sine_rows(width):
    k = np.arange(1, width + 1)
    phases = k[:, None] * k[None, :] % (2 * (width + 1))
    return math.sqrt(2.0 / (width + 1)) * np.sin(phases * (math.pi / (width + 1)))


def eigen_first(wavenumber, width):
    return 4.0 * jnp.square(jnp.sin(wavenumber.astype(jnp.float32) * (math.pi / (2 * width))))


def eigen_second(width):
    wavenumber = jnp.arange(1, width + 1, dtype=jnp.int32).astype(jnp.float32)
    return 4.0 * jnp.square(jnp.sin(wavenumber * (math.pi / (2 * (width + 1)))))


def split(x):
    high = x.astype(jnp.bfloat16)
    return high, (x - high.astype(jnp.float32)).astype(jnp.bfloat16)


def dot3(a, b, dims):
    dot = functools.partial(
        lax.dot_general, dimension_numbers=(dims, ((), ())), preferred_element_type=jnp.float32
    )
    return dot(a[0], b[0]) + dot(a[1], b[0]) + dot(a[0], b[1])


def swap_groups(blocks, group):
    n = len(blocks)
    lanes = n * group
    lane = lax.broadcasted_iota(jnp.int32, blocks[0].shape, 1)
    blocks = list(blocks)
    d = 1
    while d < n:
        keep = (lane & (d * group)) == 0
        for i in range(n):
            if i & d:
                continue
            a, b = blocks[i], blocks[i + d]
            blocks[i] = jnp.where(keep, a, pltpu.roll(b, d * group, 1))
            blocks[i + d] = jnp.where(keep, pltpu.roll(a, lanes - d * group, 1), b)
        d *= 2
    return blocks


def forward_x(src_ref, wid_ref, ch_ref, cl_ref, out_ref, acc_ref, *, devices, group):
    depth, rows, _ = src_ref.shape
    parts = rows // group
    owned = ch_ref.shape[0] // devices
    stride = owned * parts + 1
    x = jnp.concatenate(
        [src_ref[z, pl.ds(m * group, group), :] for m in range(parts) for z in range(depth)], 0
    )
    acc_ref[...] = dot3((ch_ref[...], cl_ref[...]), split(x), ((1,), (1,)))
    widths = jnp.broadcast_to(wid_ref[...], (SUB, LANES))
    for t in range(devices // SUB):
        for kk in range(owned):
            for m in range(parts):
                out_ref[pl.ds(t * SUB * stride + kk * parts + m, SUB, stride=stride), :] = acc_ref[
                    pl.ds(kk * devices + t * SUB, SUB), pl.ds(m * LANES, LANES)
                ]
        out_ref[pl.ds(t * SUB * stride + owned * parts, SUB, stride=stride), :] = widths


def backward_x(msg_ref, ch_ref, cl_ref, out_ref, z_ref, *, devices, group):
    depth, rows, _ = out_ref.shape
    parts = rows // group
    owned = ch_ref.shape[0] // devices
    stride = owned * parts
    for t in range(devices // SUB):
        for kk in range(owned):
            for m in range(parts):
                z_ref[pl.ds(kk * devices + t * SUB, SUB), pl.ds(m * LANES, LANES)] = msg_ref[
                    pl.ds(t * SUB * stride + kk * parts + m, SUB, stride=stride), :
                ]
    y = dot3(split(z_ref[...].T), (ch_ref[...], cl_ref[...]), ((1,), (0,)))
    for m in range(parts):
        for z in range(depth):
            out_ref[z, pl.ds(m * group, group), :] = y[(m * depth + z) * group :][:group]


def middle(
    msg_ref, sh_ref, sl_ref, ek_ref, el_ref, out_ref, a_ref, wid_ref, left_ref, right_ref, red_ref,
    *, peers, blocks, depth, parts, group, tile
):
    owned = ek_ref.shape[0]
    wide = el_ref.shape[1]
    stride_in, stride_out = owned * parts + 1, owned * parts
    halfs = peers // depth
    rows = depth * blocks
    cells = wide // LANES
    pitch = -(-owned * cells // SUB) * SUB

    def where(kk, zi):
        return pl.ds(kk * rows + zi * blocks, blocks)

    wid_ref[...] = jnp.zeros(wid_ref.shape, jnp.float32)
    wid_ref[pl.ds(SUB, blocks), :] = msg_ref[pl.ds(stride_in - 1, blocks, stride=stride_in), :]
    width = wid_ref[pl.ds(SUB, blocks), :]
    before, after = wid_ref[pl.ds(SUB - 1, blocks), :], wid_ref[pl.ds(SUB + 1, blocks), :]
    column = lambda a, i: a[:, i : i + 1]
    width_of = [column(width, i) for i in range(depth)]
    padded = [column(before, depth - 1), *width_of, column(after, 0)]
    link = [2.0 / (padded[i] + padded[i + 1]) for i in range(depth + 1)]
    lower, upper = link[:-1], link[1:]

    for kk in range(owned):
        for m in range(parts):
            for h in range(halfs):
                got = [
                    msg_ref[
                        pl.ds((h * depth + g) * blocks * stride_in + kk * parts + m, blocks, stride=stride_in), :
                    ]
                    for g in range(depth)
                ]
                for zi, block in enumerate(swap_groups(got, group)):
                    a_ref[where(kk, zi), pl.ds((m * halfs + h) * LANES, LANES)] = block
    table = (sh_ref[...], sl_ref[...])
    a_ref[...] = dot3(split(a_ref[...]), table, ((1,), (0,)))

    def scatter(index, kk, t, value):
        for s in range(blocks // SUB):
            for c in range(tile // LANES):
                row = s * SUB * pitch + kk * cells + t * (tile // LANES) + c
                red_ref[index, pl.ds(row, SUB, stride=pitch), :] = value[
                    s * SUB : s * SUB + SUB, c * LANES : c * LANES + LANES
                ]

    for kk in range(owned):
        for t in range(wide // tile):
            cols = pl.ds(t * tile, tile)
            eigen = ek_ref[kk : kk + 1, :] + el_ref[:, cols]
            diagonal = lambda i: (lower[i] + upper[i]) + width_of[i] * eigen
            forcing = lambda i: width_of[i] * a_ref[where(kk, i), cols]
            left, right, value = [None], [None], [None]
            for i in range(1, depth):
                if i == 1:
                    inverse = 1.0 / diagonal(i)
                    left.append(-(inverse * lower[i]))
                    value.append(inverse * forcing(i))
                else:
                    inverse = 1.0 / (diagonal(i) + lower[i] * right[-1])
                    below = inverse * lower[i]
                    left.append(below * left[-1])
                    value.append(inverse * forcing(i) + below * value[-1])
                right.append(-(inverse * upper[i]))
                if i < depth - 1:
                    left_ref[where(kk, i), cols] = left[i]
                    right_ref[where(kk, i), cols] = right[i]
                    a_ref[where(kk, i), cols] = value[i]
            inner_left, inner_right, inner = left[depth - 2], right[depth - 2], value[depth - 2]
            for i in range(depth - 3, 0, -1):
                inner_left = left[i] - right[i] * inner_left
                inner_right = -(right[i] * inner_right)
                inner = value[i] - right[i] * inner
            inverse = 1.0 / (diagonal(0) + upper[0] * inner_left)
            scatter(0, kk, t, -(inverse * lower[0]))
            scatter(1, kk, t, inverse * upper[0] * inner_right)
            scatter(2, kk, t, inverse * (forcing(0) + upper[0] * inner))
            scatter(3, kk, t, left[depth - 1])
            scatter(4, kk, t, right[depth - 1])
            scatter(5, kk, t, value[depth - 1])

    ratio = rhs = None
    for q in range(blocks):
        at = pl.ds(q * pitch, pitch)
        head_below, head_above, head_in, tail_below, tail_above, tail_in = (
            red_ref[i, at, :] for i in range(6)
        )
        if q == 0:
            head_ratio, head_rhs = head_above, head_in
        else:
            divided = 1.0 / (1.0 - head_below * ratio)
            head_ratio = head_above * divided
            head_rhs = (head_in - head_below * rhs) * divided
        divided = 1.0 / (1.0 - tail_below * head_ratio)
        ratio = tail_above * divided
        rhs = (tail_in - tail_below * head_rhs) * divided
        for i, value in ((1, head_ratio), (2, head_rhs), (4, ratio), (5, rhs)):
            red_ref[i, at, :] = value
    following = None
    for q in range(blocks - 1, -1, -1):
        at = pl.ds(q * pitch, pitch)
        tail = red_ref[5, at, :]
        if following is not None:
            tail = tail - red_ref[4, at, :] * following
        following = red_ref[2, at, :] - red_ref[1, at, :] * tail
        red_ref[0, at, :] = following
        red_ref[3, at, :] = tail

    for kk in range(owned):
        for s in range(blocks // SUB):
            for c in range(cells):
                row = s * SUB * pitch + kk * cells + c
                cols = pl.ds(c * LANES, LANES)
                for zi, index in ((0, 0), (depth - 1, 3)):
                    a_ref[pl.ds(kk * rows + zi * blocks + s * SUB, SUB), cols] = red_ref[
                        index, pl.ds(row, SUB, stride=pitch), :
                    ]
        for t in range(wide // tile):
            cols = pl.ds(t * tile, tile)
            head, following = a_ref[where(kk, 0), cols], a_ref[where(kk, depth - 1), cols]
            for i in range(depth - 2, 0, -1):
                at = where(kk, i)
                following = (a_ref[at, cols] - left_ref[at, cols] * head) - right_ref[at, cols] * following
                a_ref[at, cols] = following

    a_ref[...] = dot3(split(a_ref[...]), table, ((1,), (1,)))
    for kk in range(owned):
        for m in range(parts):
            for h in range(halfs):
                lanes = pl.ds((m * halfs + h) * LANES, LANES)
                sent = swap_groups([a_ref[where(kk, zi), lanes] for zi in range(depth)], group)
                for g, block in enumerate(sent):
                    row = (h * depth + g) * blocks * stride_out + kk * parts + m
                    out_ref[pl.ds(row, blocks, stride=stride_out), :] = block


def call(kernel, name, out, args, scratch):
    return pl.pallas_call(
        kernel,
        name=name,
        out_shape=jax.ShapeDtypeStruct(out, jnp.float32),
        in_specs=[pl.BlockSpec(memory_space=VMEM)] * len(args),
        out_specs=pl.BlockSpec(memory_space=VMEM),
        scratch_shapes=[pltpu.VMEM(s, jnp.float32) for s in scratch],
    )(*args)


def exchange(rows, devices):
    flat = rows.reshape(devices, 1, -1)
    return lax.all_to_all(flat, ALL, split_axis=0, concat_axis=0, tiled=True).reshape(-1, LANES)


def on_device(source, cell_width):
    depth, rows, width_x = source.shape
    peers, blocks = lax.axis_size("pa"), lax.axis_size("gz")
    devices = peers * blocks
    width_y = rows * peers
    owned = width_x // devices
    group = LANES // depth
    parts = rows // group

    cosines = halves(cosine_rows(width_x))
    order = np.arange(width_y).reshape(peers, parts, group).transpose(1, 0, 2).reshape(-1)
    sines = halves(sine_rows(width_y)[order])
    widths = jnp.pad(cell_width, (0, LANES - depth))[None]
    sent = call(
        functools.partial(forward_x, devices=devices, group=group), "forward_x",
        (devices * (owned * parts + 1), LANES), (source, widths, *cosines),
        [(width_x, depth * rows)],
    )
    own_k = jnp.arange(owned, dtype=jnp.int32) * devices + lax.axis_index(ALL)
    eigen_x, eigen_y = eigen_first(own_k, width_x)[:, None], eigen_second(width_y)[None]
    cells = width_y // LANES
    pitch = -(-owned * cells // SUB) * SUB
    size = (owned * depth * blocks, width_y)
    back = call(
        functools.partial(
            middle, peers=peers, blocks=blocks, depth=depth, parts=parts, group=group, tile=TILE
        ),
        "middle", (devices * owned * parts, LANES),
        (exchange(sent, devices), *sines, eigen_x, eigen_y),
        [size, (blocks + 2 * SUB, LANES), size, size, (6, blocks * pitch, LANES)],
    )
    return call(
        functools.partial(backward_x, devices=devices, group=group), "backward_x", source.shape,
        (exchange(back, devices), *cosines), [(width_x, depth * rows)],
    )


TILE = 384


def solution(mesh):
    return jax.shard_map(
        on_device,
        mesh=mesh,
        in_specs=(P("gz", "pa", None), P("gz")),
        out_specs=P("gz", "pa", None),
        check_vma=False,
    )
```

```python
import functools
import math

import numpy as np

import jax
import jax.numpy as jnp
from jax import lax
from jax.experimental import pallas as pl
from jax.experimental.pallas import tpu as pltpu
from jax.sharding import PartitionSpec as P

ALL = ("pa", "gz")
LANES = 128
SUB = 8
VMEM = pltpu.MemorySpace.VMEM


def halves(table):
    table = table.astype(np.float32)
    high = table.astype(jnp.bfloat16)
    low = (table - high.astype(np.float32)).astype(jnp.bfloat16)
    return jnp.asarray(high), jnp.asarray(low)


def cosine_rows(width):
    k = np.arange(width)
    phases = k[:, None] * (2 * k[None, :] + 1) % (4 * width)
    weights = np.where(k == 0, math.sqrt(1.0 / width), math.sqrt(2.0 / width))
    return weights[:, None] * np.cos(phases * (math.pi / (2 * width)))


def sine_rows(width):
    k = np.arange(1, width + 1)
    phases = k[:, None] * k[None, :] % (2 * (width + 1))
    return math.sqrt(2.0 / (width + 1)) * np.sin(phases * (math.pi / (width + 1)))


def eigen_first(wavenumber, width):
    return 4.0 * jnp.square(jnp.sin(wavenumber.astype(jnp.float32) * (math.pi / (2 * width))))


def eigen_second(width):
    wavenumber = jnp.arange(1, width + 1, dtype=jnp.int32).astype(jnp.float32)
    return 4.0 * jnp.square(jnp.sin(wavenumber * (math.pi / (2 * (width + 1)))))


def split(x):
    high = x.astype(jnp.bfloat16)
    return high, (x - high.astype(jnp.float32)).astype(jnp.bfloat16)


def dot3(a, b, dims):
    lhs = jnp.concatenate([a[0], a[1], a[0]], dims[0][0])
    rhs = jnp.concatenate([b[0], b[0], b[1]], dims[1][0])
    return lax.dot_general(lhs, rhs, (dims, ((), ())), preferred_element_type=jnp.float32)


def swap_groups(blocks, group):
    n = len(blocks)
    lanes = n * group
    lane = lax.broadcasted_iota(jnp.int32, blocks[0].shape, 1)
    blocks = list(blocks)
    d = 1
    while d < n:
        keep = (lane & (d * group)) == 0
        for i in range(n):
            if i & d:
                continue
            a, b = blocks[i], blocks[i + d]
            blocks[i] = jnp.where(keep, a, pltpu.roll(b, d * group, 1))
            blocks[i + d] = jnp.where(keep, pltpu.roll(a, lanes - d * group, 1), b)
        d *= 2
    return blocks


def forward_x(src_ref, ch_ref, cl_ref, out_ref, xh_ref, xl_ref, acc_ref, *, group):
    depth, rows, width = src_ref.shape
    parts = rows // group
    owned, some, _ = ch_ref.shape
    stride = owned * parts

    @pl.when(pl.program_id(0) == 0)
    def _():
        for m in range(parts):
            for z in range(depth):
                at = pl.ds((m * depth + z) * group, group)
                xh_ref[at, :], xl_ref[at, :] = split(src_ref[z, pl.ds(m * group, group), :])

    table = (ch_ref[...].reshape(owned * some, width), cl_ref[...].reshape(owned * some, width))
    acc_ref[...] = dot3(table, (xh_ref[...], xl_ref[...]), ((1,), (1,)))
    for t in range(some // SUB):
        for kk in range(owned):
            for m in range(parts):
                out_ref[pl.ds(t * SUB * stride + kk * parts + m, SUB, stride=stride), :] = acc_ref[
                    pl.ds(kk * some + t * SUB, SUB), pl.ds(m * LANES, LANES)
                ]


def backward_x(msg_ref, ch_ref, cl_ref, out_ref, z_ref, zh_ref, zl_ref, *, group):
    depth, rows, _ = out_ref.shape
    parts = rows // group
    owned, devices, some = ch_ref.shape
    stride = owned * parts
    table = [ref[...].reshape(owned * devices, some) for ref in (ch_ref, cl_ref)]

    @pl.when(pl.program_id(0) == 0)
    def _():
        for t in range(devices // SUB):
            for kk in range(owned):
                for m in range(parts):
                    z_ref[pl.ds(kk * devices + t * SUB, SUB), pl.ds(m * LANES, LANES)] = msg_ref[
                        pl.ds(t * SUB * stride + kk * parts + m, SUB, stride=stride), :
                    ]
        zh_ref[...], zl_ref[...] = split(z_ref[...].T)

    y = dot3((zh_ref[...], zl_ref[...]), table, ((1,), (0,)))
    for m in range(parts):
        for z in range(depth):
            out_ref[z, pl.ds(m * group, group), :] = y[(m * depth + z) * group :][:group]


def coefficients(wid_in_ref, ek_ref, el_ref, cell_ref, block_ref, wid_ref, red_ref, *, depth, tile):
    blocks = wid_in_ref.shape[0]
    owned, wide = ek_ref.shape[0], el_ref.shape[1]
    rows = depth * blocks
    cells = wide // LANES
    pitch = -(-owned * cells // SUB) * SUB

    wid_ref[...] = jnp.zeros(wid_ref.shape, jnp.float32)
    wid_ref[pl.ds(SUB, blocks), :] = wid_in_ref[...]
    width = wid_ref[pl.ds(SUB, blocks), :]
    before, after = wid_ref[pl.ds(SUB - 1, blocks), :], wid_ref[pl.ds(SUB + 1, blocks), :]
    column = lambda a, i: a[:, i : i + 1]
    width_of = [column(width, i) for i in range(depth)]
    padded = [column(before, depth - 1), *width_of, column(after, 0)]
    link = [2.0 / (padded[i] + padded[i + 1]) for i in range(depth + 1)]
    lower, upper = link[:-1], link[1:]
    red_ref[...] = jnp.zeros(red_ref.shape, jnp.float32)

    def scatter(index, kk, t, value):
        for s in range(blocks // SUB):
            for c in range(tile // LANES):
                row = s * SUB * pitch + kk * cells + t * (tile // LANES) + c
                red_ref[index, pl.ds(row, SUB, stride=pitch), :] = value[
                    s * SUB : s * SUB + SUB, c * LANES : c * LANES + LANES
                ]

    for kk in range(owned):
        for t in range(wide // tile):
            cols = pl.ds(t * tile, tile)
            eigen = ek_ref[kk : kk + 1, :] + el_ref[:, cols]
            diagonal = lambda i: (lower[i] + upper[i]) + width_of[i] * eigen
            left, right = [None], [None]
            for i in range(1, depth):
                if i == 1:
                    inverse = 1.0 / diagonal(i)
                    below = jnp.zeros(inverse.shape, jnp.float32)
                    left.append(-(inverse * lower[i]))
                else:
                    inverse = 1.0 / (diagonal(i) + lower[i] * right[-1])
                    below = inverse * lower[i]
                    left.append(below * left[-1])
                right.append(-(inverse * upper[i]))
                at = pl.ds(kk * rows + i * blocks, blocks)
                for index, value in enumerate((inverse * width_of[i], below, left[i], right[i])):
                    cell_ref[index, at, cols] = value
            inner_left, inner_right = left[depth - 2], right[depth - 2]
            for i in range(depth - 3, 0, -1):
                inner_left = left[i] - right[i] * inner_left
                inner_right = -(right[i] * inner_right)
            inverse = 1.0 / (diagonal(0) + upper[0] * inner_left)
            at = pl.ds(kk * rows, blocks)
            above = inverse * upper[0]
            zero = jnp.zeros(inverse.shape, jnp.float32)
            for index, value in enumerate((inverse * width_of[0], above, zero, zero)):
                cell_ref[index, at, cols] = value
            scatter(0, kk, t, -(inverse * lower[0]))
            scatter(1, kk, t, above * inner_right)
            scatter(2, kk, t, left[depth - 1])
            scatter(3, kk, t, right[depth - 1])

    ratio = None
    for q in range(blocks):
        at = pl.ds(q * pitch, pitch)
        head_below, head_above, tail_below, tail_above = (red_ref[i, at, :] for i in range(4))
        if q == 0:
            head_own = jnp.ones(head_above.shape, jnp.float32)
            head_up = jnp.zeros(head_above.shape, jnp.float32)
            head_ratio = head_above
        else:
            head_own = 1.0 / (1.0 - head_below * ratio)
            head_up = -(head_below * head_own)
            head_ratio = head_above * head_own
        tail_own = 1.0 / (1.0 - tail_below * head_ratio)
        ratio = tail_above * tail_own
        found = (head_own, head_up, tail_own, -(tail_below * tail_own), head_ratio, ratio)
        for index, value in enumerate(found):
            block_ref[index, at, :] = value


def middle(
    msg_ref, sh_in, sl_in, cell_in, block_in, out_ref, a_ref, red_ref, sh_ref, sl_ref, cell_ref, block_ref, sems,
    *, peers, blocks, depth, parts, group, owned, tile
):
    copies = [
        pltpu.make_async_copy(source, target, sems.at[i])
        for i, (source, target) in enumerate(
            ((sh_in, sh_ref), (sl_in, sl_ref), (cell_in, cell_ref), (block_in, block_ref))
        )
    ]
    for copy in copies:
        copy.start()
    wide = sh_in.shape[1]
    stride = owned * parts
    halfs = peers // depth
    rows = depth * blocks
    cells = wide // LANES
    pitch = -(-owned * cells // SUB) * SUB

    def where(kk, zi):
        return pl.ds(kk * rows + zi * blocks, blocks)

    for kk in range(owned):
        for m in range(parts):
            for h in range(halfs):
                got = [
                    msg_ref[pl.ds((h * depth + g) * blocks * stride + kk * parts + m, blocks, stride=stride), :]
                    for g in range(depth)
                ]
                for zi, block in enumerate(swap_groups(got, group)):
                    a_ref[where(kk, zi), pl.ds((m * halfs + h) * LANES, LANES)] = block
    copies[0].wait()
    copies[1].wait()
    table = (sh_ref[...], sl_ref[...])
    for kk in range(owned):
        at = pl.ds(kk * rows, rows)
        a_ref[at, :] = dot3(split(a_ref[at, :]), table, ((1,), (0,)))
    copies[2].wait()
    copies[3].wait()

    def scatter(index, kk, t, value):
        for s in range(blocks // SUB):
            for c in range(tile // LANES):
                row = s * SUB * pitch + kk * cells + t * (tile // LANES) + c
                red_ref[index, pl.ds(row, SUB, stride=pitch), :] = value[
                    s * SUB : s * SUB + SUB, c * LANES : c * LANES + LANES
                ]

    red_ref[...] = jnp.zeros(red_ref.shape, jnp.float32)
    for kk in range(owned):
        for t in range(wide // tile):
            cols = pl.ds(t * tile, tile)
            value = [None]
            for i in range(1, depth):
                at = where(kk, i)
                now = cell_ref[0, at, cols] * a_ref[at, cols]
                if i > 1:
                    now = now + cell_ref[1, at, cols] * value[-1]
                value.append(now)
                if i < depth - 1:
                    a_ref[at, cols] = now
            inner = value[depth - 2]
            for i in range(depth - 3, 0, -1):
                inner = value[i] - cell_ref[3, where(kk, i), cols] * inner
            at = where(kk, 0)
            scatter(0, kk, t, cell_ref[0, at, cols] * a_ref[at, cols] + cell_ref[1, at, cols] * inner)
            scatter(1, kk, t, value[depth - 1])

    rhs = None
    for q in range(blocks):
        at = pl.ds(q * pitch, pitch)
        head = block_ref[0, at, :] * red_ref[0, at, :]
        if rhs is not None:
            head = head + block_ref[1, at, :] * rhs
        rhs = block_ref[2, at, :] * red_ref[1, at, :] + block_ref[3, at, :] * head
        red_ref[0, at, :] = head
        red_ref[1, at, :] = rhs
    following = None
    for q in range(blocks - 1, -1, -1):
        at = pl.ds(q * pitch, pitch)
        tail = red_ref[1, at, :]
        if following is not None:
            tail = tail - block_ref[5, at, :] * following
            red_ref[1, at, :] = tail
        following = red_ref[0, at, :] - block_ref[4, at, :] * tail
        red_ref[0, at, :] = following

    for kk in range(owned):
        for s in range(blocks // SUB):
            for c in range(cells):
                row = s * SUB * pitch + kk * cells + c
                cols = pl.ds(c * LANES, LANES)
                for zi, index in ((0, 0), (depth - 1, 1)):
                    a_ref[pl.ds(kk * rows + zi * blocks + s * SUB, SUB), cols] = red_ref[
                        index, pl.ds(row, SUB, stride=pitch), :
                    ]
        for t in range(wide // tile):
            cols = pl.ds(t * tile, tile)
            head, following = a_ref[where(kk, 0), cols], a_ref[where(kk, depth - 1), cols]
            for i in range(depth - 2, 0, -1):
                at = where(kk, i)
                free = a_ref[at, cols] - cell_ref[2, at, cols] * head
                following = free - cell_ref[3, at, cols] * following
                a_ref[at, cols] = following
        at = pl.ds(kk * rows, rows)
        a_ref[at, :] = dot3(split(a_ref[at, :]), table, ((1,), (1,)))
        for m in range(parts):
            for h in range(halfs):
                lanes = pl.ds((m * halfs + h) * LANES, LANES)
                sent = swap_groups([a_ref[where(kk, zi), lanes] for zi in range(depth)], group)
                for g, block in enumerate(sent):
                    row = (h * depth + g) * blocks * stride + kk * parts + m
                    out_ref[pl.ds(row, blocks, stride=stride), :] = block


WHOLE = pl.BlockSpec(memory_space=VMEM)
STEPS = 2


def call_forward(source, high, low, group):
    depth, rows, width = source.shape
    owned, devices, _ = high.shape
    some = devices // STEPS
    table = pl.BlockSpec((owned, some, width), lambda j: (0, j, 0))
    out = width * depth * rows // LANES
    return pl.pallas_call(
        functools.partial(forward_x, group=group),
        name="forward_x",
        grid=(STEPS,),
        out_shape=jax.ShapeDtypeStruct((out, LANES), jnp.float32),
        in_specs=[pl.BlockSpec(source.shape, lambda j: (0, 0, 0)), table, table],
        out_specs=pl.BlockSpec((out // STEPS, LANES), lambda j: (j, 0)),
        scratch_shapes=[
            pltpu.VMEM((depth * rows, width), jnp.bfloat16),
            pltpu.VMEM((depth * rows, width), jnp.bfloat16),
            pltpu.VMEM((owned * some, depth * rows), jnp.float32),
        ],
    )(source, high, low)


def call_backward(message, high, low, shape, group):
    depth, rows, width = shape
    steps = width // 256
    table = pl.BlockSpec((*high.shape[:2], width // steps), lambda j: (0, 0, j))
    return pl.pallas_call(
        functools.partial(backward_x, group=group),
        name="backward_x",
        grid=(steps,),
        out_shape=jax.ShapeDtypeStruct(shape, jnp.float32),
        in_specs=[pl.BlockSpec(message.shape, lambda j: (0, 0)), table, table],
        out_specs=pl.BlockSpec((depth, rows, width // steps), lambda j: (0, 0, j)),
        scratch_shapes=[
            pltpu.VMEM((width, depth * rows), jnp.float32),
            pltpu.VMEM((depth * rows, width), jnp.bfloat16),
            pltpu.VMEM((depth * rows, width), jnp.bfloat16),
        ],
    )(message, high, low)


def call_coefficients(widths, eigen_x, eigen_y, depth):
    blocks, owned, wide = widths.shape[0], eigen_x.shape[0], eigen_y.shape[1]
    pitch = -(-owned * (wide // LANES) // SUB) * SUB
    shapes = ((4, owned * depth * blocks, wide), (6, blocks * pitch, LANES))
    return pl.pallas_call(
        functools.partial(coefficients, depth=depth, tile=wide // 2),
        name="coefficients",
        out_shape=[jax.ShapeDtypeStruct(s, jnp.float32) for s in shapes],
        in_specs=[WHOLE] * 3,
        out_specs=[WHOLE] * 2,
        scratch_shapes=[
            pltpu.VMEM((blocks + 2 * SUB, LANES), jnp.float32),
            pltpu.VMEM((4, blocks * pitch, LANES), jnp.float32),
        ],
    )(widths, eigen_x, eigen_y)


def call_middle(message, high, low, cell, block, *, peers, blocks, depth, parts, group, owned):
    wide = high.shape[1]
    anywhere = pl.BlockSpec(memory_space=pl.ANY)
    return pl.pallas_call(
        functools.partial(
            middle, peers=peers, blocks=blocks, depth=depth, parts=parts, group=group, owned=owned, tile=wide // 2
        ),
        name="middle",
        out_shape=jax.ShapeDtypeStruct(message.shape, jnp.float32),
        in_specs=[WHOLE, *[anywhere] * 4],
        out_specs=WHOLE,
        scratch_shapes=[
            pltpu.VMEM((owned * depth * blocks, wide), jnp.float32),
            pltpu.VMEM((2, *block.shape[1:]), jnp.float32),
            pltpu.VMEM(high.shape, jnp.bfloat16),
            pltpu.VMEM(low.shape, jnp.bfloat16),
            pltpu.VMEM(cell.shape, jnp.float32),
            pltpu.VMEM(block.shape, jnp.float32),
            pltpu.SemaphoreType.DMA((4,)),
        ],
    )(message, high, low, cell, block)


def exchange(rows, devices):
    flat = rows.reshape(devices, 1, -1)
    return lax.all_to_all(flat, ALL, split_axis=0, concat_axis=0, tiled=True).reshape(-1, LANES)


def all_widths(cell_width, blocks):
    depth = cell_width.shape[0]
    row = lax.broadcasted_iota(jnp.int32, (blocks, LANES), 0)
    held = jnp.where(row == lax.axis_index("gz"), jnp.pad(cell_width, (0, LANES - depth))[None], 0.0)
    step = 1
    while step < blocks:
        held = held + lax.ppermute(held, "gz", [(i, i ^ step) for i in range(blocks)])
        step *= 2
    return held


def on_device(source, cell_width):
    depth, rows, width_x = source.shape
    peers, blocks = lax.axis_size("pa"), lax.axis_size("gz")
    devices = peers * blocks
    width_y = rows * peers
    owned = width_x // devices
    group = LANES // depth
    parts = rows // group

    cosines = halves(cosine_rows(width_x).reshape(owned, devices, width_x))
    order = np.arange(width_y).reshape(peers, parts, group).transpose(1, 0, 2).reshape(-1)
    sines = halves(sine_rows(width_y)[order])
    got = exchange(call_forward(source, *cosines, group), devices)

    own_k = jnp.arange(owned, dtype=jnp.int32) * devices + lax.axis_index(ALL)
    eigen_x, eigen_y = eigen_first(own_k, width_x)[:, None], eigen_second(width_y)[None]
    solve = call_coefficients(all_widths(cell_width, blocks), eigen_x, eigen_y, depth)
    back = call_middle(
        got, *sines, *solve,
        peers=peers, blocks=blocks, depth=depth, parts=parts, group=group, owned=owned,
    )
    return call_backward(exchange(back, devices), *cosines, source.shape, group)


def solution(mesh):
    return jax.shard_map(
        on_device,
        mesh=mesh,
        in_specs=(P("gz", "pa", None), P("gz")),
        out_specs=P("gz", "pa", None),
        check_vma=False,
    )
```

```python
import functools
import math

import numpy as np

import jax
import jax.numpy as jnp
from jax import lax
from jax.experimental import pallas as pl
from jax.experimental.pallas import tpu as pltpu
from jax.sharding import PartitionSpec as P

ALL = ("pa", "gz")
LANES = 128
SUB = 8
VMEM = pltpu.MemorySpace.VMEM


def halves(table):
    table = table.astype(np.float32)
    high = table.astype(jnp.bfloat16)
    low = (table - high.astype(np.float32)).astype(jnp.bfloat16)
    return jnp.asarray(high), jnp.asarray(low)


def cosine_rows(width):
    k = np.arange(width)
    phases = k[:, None] * (2 * k[None, :] + 1) % (4 * width)
    weights = np.where(k == 0, math.sqrt(1.0 / width), math.sqrt(2.0 / width))
    return weights[:, None] * np.cos(phases * (math.pi / (2 * width)))


def sine_rows(width):
    k = np.arange(1, width + 1)
    phases = k[:, None] * k[None, :] % (2 * (width + 1))
    return math.sqrt(2.0 / (width + 1)) * np.sin(phases * (math.pi / (width + 1)))


def eigen_first(wavenumber, width):
    return 4.0 * jnp.square(jnp.sin(wavenumber.astype(jnp.float32) * (math.pi / (2 * width))))


def eigen_second(width):
    wavenumber = jnp.arange(1, width + 1, dtype=jnp.int32).astype(jnp.float32)
    return 4.0 * jnp.square(jnp.sin(wavenumber * (math.pi / (2 * (width + 1)))))


def split(x):
    high = x.astype(jnp.bfloat16)
    return high, (x - high.astype(jnp.float32)).astype(jnp.bfloat16)


def dot3(a, b, dims):
    lhs = jnp.concatenate([a[0], a[1], a[0]], dims[0][0])
    rhs = jnp.concatenate([b[0], b[0], b[1]], dims[1][0])
    return lax.dot_general(lhs, rhs, (dims, ((), ())), preferred_element_type=jnp.float32)


def swap_groups(blocks, group):
    n = len(blocks)
    lanes = n * group
    lane = lax.broadcasted_iota(jnp.int32, blocks[0].shape, 1)
    blocks = list(blocks)
    d = 1
    while d < n:
        keep = (lane & (d * group)) == 0
        for i in range(n):
            if i & d:
                continue
            a, b = blocks[i], blocks[i + d]
            blocks[i] = jnp.where(keep, a, pltpu.roll(b, d * group, 1))
            blocks[i + d] = jnp.where(keep, pltpu.roll(a, lanes - d * group, 1), b)
        d *= 2
    return blocks


def forward_x(src_ref, ch_ref, cl_ref, out_ref, acc_ref, *, group):
    depth, rows, some = src_ref.shape
    parts = rows // group
    owned, devices, _ = ch_ref.shape
    stride = owned * parts
    step = pl.program_id(0)
    x = jnp.concatenate(
        [src_ref[z, pl.ds(m * group, group), :] for m in range(parts) for z in range(depth)], 0
    )
    table = [ref[...].reshape(owned * devices, some) for ref in (ch_ref, cl_ref)]
    part = dot3(table, split(x), ((1,), (1,)))

    @pl.when(step == 0)
    def _():
        acc_ref[...] = part

    @pl.when(step > 0)
    def _():
        acc_ref[...] += part

    @pl.when(step == pl.num_programs(0) - 1)
    def _():
        for t in range(devices // SUB):
            for kk in range(owned):
                for m in range(parts):
                    out_ref[pl.ds(t * SUB * stride + kk * parts + m, SUB, stride=stride), :] = acc_ref[
                        pl.ds(kk * devices + t * SUB, SUB), pl.ds(m * LANES, LANES)
                    ]


def backward_x(msg_ref, ch_ref, cl_ref, out_ref, z_ref, zh_ref, zl_ref, *, group):
    depth, rows, some = out_ref.shape
    parts = rows // group
    owned, devices, _ = ch_ref.shape
    stride = owned * parts
    cols = pl.ds(pl.multiple_of(pl.program_id(0) * some, some), some)
    table = [ref[:, :, cols].reshape(owned * devices, some) for ref in (ch_ref, cl_ref)]

    @pl.when(pl.program_id(0) == 0)
    def _():
        for t in range(devices // SUB):
            for kk in range(owned):
                for m in range(parts):
                    z_ref[pl.ds(kk * devices + t * SUB, SUB), pl.ds(m * LANES, LANES)] = msg_ref[
                        pl.ds(t * SUB * stride + kk * parts + m, SUB, stride=stride), :
                    ]
        zh_ref[...], zl_ref[...] = split(z_ref[...].T)

    y = dot3((zh_ref[...], zl_ref[...]), table, ((1,), (0,)))
    for m in range(parts):
        for z in range(depth):
            out_ref[z, pl.ds(m * group, group), :] = y[(m * depth + z) * group :][:group]


def coefficients(wid_in_ref, ek_ref, el_ref, cell_ref, block_ref, wid_ref, red_ref, *, depth, tile):
    blocks = wid_in_ref.shape[0]
    owned, wide = ek_ref.shape[0], el_ref.shape[1]
    rows = depth * blocks
    cells = wide // LANES
    pitch = -(-owned * cells // SUB) * SUB

    wid_ref[...] = jnp.zeros(wid_ref.shape, jnp.float32)
    wid_ref[pl.ds(SUB, blocks), :] = wid_in_ref[...]
    width = wid_ref[pl.ds(SUB, blocks), :]
    before, after = wid_ref[pl.ds(SUB - 1, blocks), :], wid_ref[pl.ds(SUB + 1, blocks), :]
    column = lambda a, i: a[:, i : i + 1]
    width_of = [column(width, i) for i in range(depth)]
    padded = [column(before, depth - 1), *width_of, column(after, 0)]
    link = [2.0 / (padded[i] + padded[i + 1]) for i in range(depth + 1)]
    lower, upper = link[:-1], link[1:]
    red_ref[...] = jnp.zeros(red_ref.shape, jnp.float32)

    def scatter(index, kk, t, value):
        for s in range(blocks // SUB):
            for c in range(tile // LANES):
                row = s * SUB * pitch + kk * cells + t * (tile // LANES) + c
                red_ref[index, pl.ds(row, SUB, stride=pitch), :] = value[
                    s * SUB : s * SUB + SUB, c * LANES : c * LANES + LANES
                ]

    for kk in range(owned):
        for t in range(wide // tile):
            cols = pl.ds(t * tile, tile)
            eigen = ek_ref[kk : kk + 1, :] + el_ref[:, cols]
            diagonal = lambda i: (lower[i] + upper[i]) + width_of[i] * eigen
            left, right = [None], [None]
            for i in range(1, depth):
                if i == 1:
                    inverse = 1.0 / diagonal(i)
                    below = jnp.zeros(inverse.shape, jnp.float32)
                    left.append(-(inverse * lower[i]))
                else:
                    inverse = 1.0 / (diagonal(i) + lower[i] * right[-1])
                    below = inverse * lower[i]
                    left.append(below * left[-1])
                right.append(-(inverse * upper[i]))
                at = pl.ds(kk * rows + i * blocks, blocks)
                for index, value in enumerate((inverse * width_of[i], below, left[i], right[i])):
                    cell_ref[index, at, cols] = value
            inner_left, inner_right = left[depth - 2], right[depth - 2]
            for i in range(depth - 3, 0, -1):
                inner_left = left[i] - right[i] * inner_left
                inner_right = -(right[i] * inner_right)
            inverse = 1.0 / (diagonal(0) + upper[0] * inner_left)
            at = pl.ds(kk * rows, blocks)
            above = inverse * upper[0]
            zero = jnp.zeros(inverse.shape, jnp.float32)
            for index, value in enumerate((inverse * width_of[0], above, zero, zero)):
                cell_ref[index, at, cols] = value
            scatter(0, kk, t, -(inverse * lower[0]))
            scatter(1, kk, t, above * inner_right)
            scatter(2, kk, t, left[depth - 1])
            scatter(3, kk, t, right[depth - 1])

    ratio = None
    for q in range(blocks):
        at = pl.ds(q * pitch, pitch)
        head_below, head_above, tail_below, tail_above = (red_ref[i, at, :] for i in range(4))
        if q == 0:
            head_own = jnp.ones(head_above.shape, jnp.float32)
            head_up = jnp.zeros(head_above.shape, jnp.float32)
            head_ratio = head_above
        else:
            head_own = 1.0 / (1.0 - head_below * ratio)
            head_up = -(head_below * head_own)
            head_ratio = head_above * head_own
        tail_own = 1.0 / (1.0 - tail_below * head_ratio)
        ratio = tail_above * tail_own
        found = (head_own, head_up, tail_own, -(tail_below * tail_own), head_ratio, ratio)
        for index, value in enumerate(found):
            block_ref[index, at, :] = value


def middle(
    msg_ref, sh_ref, sl_ref, cell_in, block_in, out_ref, a_ref, xh_ref, xl_ref, red_ref, cell_ref, block_ref, sems,
    *, peers, blocks, depth, parts, group, owned, tile
):
    copies = [
        pltpu.make_async_copy(source, target, sems.at[i])
        for i, (source, target) in enumerate(((cell_in, cell_ref), (block_in, block_ref)))
    ]
    for copy in copies:
        copy.start()
    wide = sh_ref.shape[1]
    stride = owned * parts
    halfs = peers // depth
    rows = depth * blocks
    cells = wide // LANES
    pitch = -(-owned * cells // SUB) * SUB

    def each(count, body):
        lax.fori_loop(0, count, lambda i, _: (body(i), 0)[1], 0)

    def where(kk, zi):
        return pl.ds(pl.multiple_of(kk * rows + zi * blocks, blocks), blocks)

    def slot(kk, m, g, h):
        return pl.ds((h * depth + g) * blocks * stride + kk * parts + m, blocks, stride=stride)

    def gather(kk):
        for m in range(parts):
            for h in range(halfs):
                got = [msg_ref[slot(kk, m, g, h), :] for g in range(depth)]
                lanes = pl.ds((m * halfs + h) * LANES, LANES)
                for zi, block in enumerate(swap_groups(got, group)):
                    at = where(kk, zi)
                    xh_ref[at, lanes], xl_ref[at, lanes] = split(block)

    each(owned, gather)

    def transform(j):
        cols = pl.ds(pl.multiple_of(j * 256, 256), 256)
        a_ref[:, cols] = dot3((xh_ref[...], xl_ref[...]), (sh_ref[:, cols], sl_ref[:, cols]), ((1,), (0,)))

    each(wide // 256, transform)
    for copy in copies:
        copy.wait()

    def scatter(index, kk, t, value):
        for s in range(blocks // SUB):
            for c in range(tile // LANES):
                row = s * SUB * pitch + kk * cells + t * (tile // LANES) + c
                red_ref[index, pl.ds(row, SUB, stride=pitch), :] = value[
                    s * SUB : s * SUB + SUB, c * LANES : c * LANES + LANES
                ]

    def reduce(kk):
        for t in range(wide // tile):
            cols = pl.ds(t * tile, tile)
            value = [None]
            for i in range(1, depth):
                at = where(kk, i)
                now = cell_ref[0, at, cols] * a_ref[at, cols]
                if i > 1:
                    now = now + cell_ref[1, at, cols] * value[-1]
                value.append(now)
                if i < depth - 1:
                    a_ref[at, cols] = now
            inner = value[depth - 2]
            for i in range(depth - 3, 0, -1):
                inner = value[i] - cell_ref[3, where(kk, i), cols] * inner
            at = where(kk, 0)
            scatter(0, kk, t, cell_ref[0, at, cols] * a_ref[at, cols] + cell_ref[1, at, cols] * inner)
            scatter(1, kk, t, value[depth - 1])

    red_ref[...] = jnp.zeros(red_ref.shape, jnp.float32)
    each(owned, reduce)

    rhs = None
    for q in range(blocks):
        at = pl.ds(q * pitch, pitch)
        head = block_ref[0, at, :] * red_ref[0, at, :]
        if rhs is not None:
            head = head + block_ref[1, at, :] * rhs
        rhs = block_ref[2, at, :] * red_ref[1, at, :] + block_ref[3, at, :] * head
        red_ref[0, at, :] = head
        red_ref[1, at, :] = rhs
    following = None
    for q in range(blocks - 1, -1, -1):
        at = pl.ds(q * pitch, pitch)
        tail = red_ref[1, at, :]
        if following is not None:
            tail = tail - block_ref[5, at, :] * following
            red_ref[1, at, :] = tail
        following = red_ref[0, at, :] - block_ref[4, at, :] * tail
        red_ref[0, at, :] = following

    def column(index, kk, t):
        return jnp.concatenate(
            [
                jnp.concatenate(
                    [
                        red_ref[index, pl.ds(s * SUB * pitch + kk * cells + t * (tile // LANES) + c, SUB, stride=pitch), :]
                        for c in range(tile // LANES)
                    ],
                    1,
                )
                for s in range(blocks // SUB)
            ],
            0,
        )

    def substitute(kk):
        for t in range(wide // tile):
            cols = pl.ds(t * tile, tile)
            head, following = column(0, kk, t), column(1, kk, t)
            for zi, value in ((0, head), (depth - 1, following)):
                at = where(kk, zi)
                xh_ref[at, cols], xl_ref[at, cols] = split(value)
            for i in range(depth - 2, 0, -1):
                at = where(kk, i)
                free = a_ref[at, cols] - cell_ref[2, at, cols] * head
                following = free - cell_ref[3, at, cols] * following
                xh_ref[at, cols], xl_ref[at, cols] = split(following)

    each(owned, substitute)

    def inverse(j):
        cols = pl.ds(pl.multiple_of(j * 256, 256), 256)
        a_ref[:, cols] = dot3((xh_ref[...], xl_ref[...]), (sh_ref[cols, :], sl_ref[cols, :]), ((1,), (1,)))

    each(wide // 256, inverse)

    def send(kk):
        for m in range(parts):
            for h in range(halfs):
                lanes = pl.ds((m * halfs + h) * LANES, LANES)
                sent = swap_groups([a_ref[where(kk, zi), lanes] for zi in range(depth)], group)
                for g, block in enumerate(sent):
                    out_ref[slot(kk, m, g, h), :] = block

    each(owned, send)


WHOLE = pl.BlockSpec(memory_space=VMEM)
PART = 256


def on_chip(*arrays):
    return [pltpu.with_memory_space_constraint(a, VMEM) for a in arrays]


def in_hbm(*arrays):
    return [pltpu.with_memory_space_constraint(a, pltpu.MemorySpace.HBM) for a in arrays]


def call_forward(source, high, low, group):
    depth, rows, width = source.shape
    table = pl.BlockSpec((*high.shape[:2], PART), lambda j: (0, 0, j))
    return pl.pallas_call(
        functools.partial(forward_x, group=group),
        name="forward_x",
        grid=(width // PART,),
        out_shape=pltpu.VMEM((width * depth * rows // LANES, LANES), jnp.float32),
        in_specs=[pl.BlockSpec((depth, rows, PART), lambda j: (0, 0, j)), table, table],
        out_specs=WHOLE,
        scratch_shapes=[pltpu.VMEM((width, depth * rows), jnp.float32)],
    )(source, high, low)


def call_backward(message, high, low, shape, group):
    depth, rows, width = shape
    return pl.pallas_call(
        functools.partial(backward_x, group=group),
        name="backward_x",
        grid=(width // PART,),
        out_shape=jax.ShapeDtypeStruct(shape, jnp.float32),
        in_specs=[WHOLE] * 3,
        out_specs=pl.BlockSpec((depth, rows, PART), lambda j: (0, 0, j)),
        scratch_shapes=[
            pltpu.VMEM((width, depth * rows), jnp.float32),
            pltpu.VMEM((depth * rows, width), jnp.bfloat16),
            pltpu.VMEM((depth * rows, width), jnp.bfloat16),
        ],
        compiler_params=pltpu.CompilerParams(vmem_limit_bytes=40 * 2**20),
    )(*on_chip(message, high, low))


def call_coefficients(widths, eigen_x, eigen_y, depth):
    blocks, owned, wide = widths.shape[0], eigen_x.shape[0], eigen_y.shape[1]
    pitch = -(-owned * (wide // LANES) // SUB) * SUB
    shapes = ((4, owned * depth * blocks, wide), (6, blocks * pitch, LANES))
    return pl.pallas_call(
        functools.partial(coefficients, depth=depth, tile=wide // 2),
        name="coefficients",
        out_shape=[jax.ShapeDtypeStruct(s, jnp.float32) for s in shapes],
        in_specs=[WHOLE] * 3,
        out_specs=[WHOLE] * 2,
        scratch_shapes=[
            pltpu.VMEM((blocks + 2 * SUB, LANES), jnp.float32),
            pltpu.VMEM((4, blocks * pitch, LANES), jnp.float32),
        ],
    )(widths, eigen_x, eigen_y)


def call_middle(message, high, low, cell, block, *, peers, blocks, depth, parts, group, owned):
    wide = high.shape[1]
    size = (owned * depth * blocks, wide)
    return pl.pallas_call(
        functools.partial(
            middle, peers=peers, blocks=blocks, depth=depth, parts=parts, group=group, owned=owned, tile=wide // 2
        ),
        name="middle",
        out_shape=pltpu.VMEM(message.shape, jnp.float32),
        in_specs=[WHOLE] * 3 + [pl.BlockSpec(memory_space=pltpu.MemorySpace.HBM)] * 2,
        out_specs=WHOLE,
        scratch_shapes=[
            pltpu.VMEM(size, jnp.float32),
            pltpu.VMEM(size, jnp.bfloat16),
            pltpu.VMEM(size, jnp.bfloat16),
            pltpu.VMEM((2, *block.shape[1:]), jnp.float32),
            pltpu.VMEM(cell.shape, jnp.float32),
            pltpu.VMEM(block.shape, jnp.float32),
            pltpu.SemaphoreType.DMA((2,)),
        ],
        compiler_params=pltpu.CompilerParams(vmem_limit_bytes=40 * 2**20),
    )(*on_chip(message, high, low), *in_hbm(cell, block))


def exchange(rows, devices):
    flat = rows.reshape(devices, 1, -1)
    return lax.all_to_all(flat, ALL, split_axis=0, concat_axis=0, tiled=True).reshape(-1, LANES)


def all_widths(cell_width, blocks):
    depth = cell_width.shape[0]
    row = lax.broadcasted_iota(jnp.int32, (blocks, LANES), 0)
    held = jnp.where(row == lax.axis_index("gz"), jnp.pad(cell_width, (0, LANES - depth))[None], 0.0)
    step = 1
    while step < blocks:
        held = held + lax.ppermute(held, "gz", [(i, i ^ step) for i in range(blocks)])
        step *= 2
    return held


def on_device(source, cell_width):
    depth, rows, width_x = source.shape
    peers, blocks = lax.axis_size("pa"), lax.axis_size("gz")
    devices = peers * blocks
    width_y = rows * peers
    owned = width_x // devices
    group = LANES // depth
    parts = rows // group

    cosines = halves(cosine_rows(width_x).reshape(owned, devices, width_x))
    order = np.arange(width_y).reshape(peers, parts, group).transpose(1, 0, 2).reshape(-1)
    sines = halves(sine_rows(width_y)[order])
    got = exchange(call_forward(source, *cosines, group), devices)

    own_k = jnp.arange(owned, dtype=jnp.int32) * devices + lax.axis_index(ALL)
    eigen_x, eigen_y = eigen_first(own_k, width_x)[:, None], eigen_second(width_y)[None]
    solve = call_coefficients(all_widths(cell_width, blocks), eigen_x, eigen_y, depth)
    back = call_middle(
        got, *sines, *solve,
        peers=peers, blocks=blocks, depth=depth, parts=parts, group=group, owned=owned,
    )
    return call_backward(exchange(back, devices), *cosines, source.shape, group)


def solution(mesh):
    return jax.shard_map(
        on_device,
        mesh=mesh,
        in_specs=(P("gz", "pa", None), P("gz")),
        out_specs=P("gz", "pa", None),
        check_vma=False,
    )
```

```python
import functools
import math

import numpy as np

import jax
import jax.numpy as jnp
from jax import lax
from jax.experimental import pallas as pl
from jax.experimental.pallas import tpu as pltpu
from jax.sharding import PartitionSpec as P

ALL = ("pa", "gz")
LANES = 128
SUB = 8
VMEM = pltpu.MemorySpace.VMEM


def halves(table):
    table = table.astype(np.float32)
    high = table.astype(jnp.bfloat16)
    low = (table - high.astype(np.float32)).astype(jnp.bfloat16)
    return jnp.asarray(high), jnp.asarray(low)


def cosine_rows(width):
    k = np.arange(width)
    phases = k[:, None] * (2 * k[None, :] + 1) % (4 * width)
    weights = np.where(k == 0, math.sqrt(1.0 / width), math.sqrt(2.0 / width))
    return weights[:, None] * np.cos(phases * (math.pi / (2 * width)))


def sine_rows(width):
    k = np.arange(1, width + 1)
    phases = k[:, None] * k[None, :] % (2 * (width + 1))
    return math.sqrt(2.0 / (width + 1)) * np.sin(phases * (math.pi / (width + 1)))


def order_y(values, peers, parts, group):
    return values.reshape(peers, parts, group).transpose(1, 0, 2).reshape(-1)


def sine_tables(peers, parts, group):
    width = peers * parts * group
    order = order_y(np.arange(width), peers, parts, group)
    return halves(sine_rows(width)[order][:, order])


def eigen_first(wavenumber, width):
    return 4.0 * jnp.square(jnp.sin(wavenumber.astype(jnp.float32) * (math.pi / (2 * width))))


def eigen_second(index, width):
    wavenumber = (index + 1).astype(jnp.float32)
    return 4.0 * jnp.square(jnp.sin(wavenumber * (math.pi / (2 * (width + 1)))))


def split(x):
    high = x.astype(jnp.bfloat16)
    return high, (x - high.astype(jnp.float32)).astype(jnp.bfloat16)


def dot3(a, b, dims):
    lhs = jnp.concatenate([a[0], a[1], a[0]], dims[0][0])
    rhs = jnp.concatenate([b[0], b[0], b[1]], dims[1][0])
    return lax.dot_general(lhs, rhs, (dims, ((), ())), preferred_element_type=jnp.float32)


def swap_groups(blocks, group):
    n = len(blocks)
    lanes = n * group
    lane = lax.broadcasted_iota(jnp.int32, blocks[0].shape, 1)
    blocks = list(blocks)
    d = 1
    while d < n:
        keep = (lane & (d * group)) == 0
        for i in range(n):
            if i & d:
                continue
            a, b = blocks[i], blocks[i + d]
            blocks[i] = jnp.where(keep, a, pltpu.roll(b, d * group, 1))
            blocks[i + d] = jnp.where(keep, pltpu.roll(a, lanes - d * group, 1), b)
        d *= 2
    return blocks


def mirrored(x):
    tiles = x.shape[1] // LANES
    lane = lax.broadcasted_iota(jnp.int32, (x.shape[0], LANES), 1)
    parts = [x[:, c * LANES : c * LANES + LANES] for c in range(tiles)]
    return jnp.concatenate([jnp.take_along_axis(p, LANES - 1 - lane, 1) for p in parts[::-1]], 1)


def start_copies(pairs, sems):
    copies = [pltpu.make_async_copy(a, b, sems.at[i]) for i, (a, b) in enumerate(pairs)]
    for copy in copies:
        copy.start()
    return copies


def forward_x(src_ref, ch_in, cl_in, out_ref, acc_ref, ch_ref, cl_ref, sems, *, owned, group):
    copies = start_copies(((ch_in, ch_ref), (cl_in, cl_ref)), sems)
    depth, rows, width = src_ref.shape
    parts = rows // group
    half = width // 2
    each = half // owned
    stride = owned * parts
    x = jnp.concatenate(
        [src_ref[z, pl.ds(m * group, group), :] for m in range(parts) for z in range(depth)], 0
    )
    near, far = x[:, :half], mirrored(x[:, half:])
    folded = split(near + far), split(near - far)
    for copy in copies:
        copy.wait()
    for odd in range(2):
        at = pl.ds(odd * half, half)
        acc_ref[at, :] = dot3((ch_ref[at, :], cl_ref[at, :]), folded[odd], ((1,), (1,)))
        for t in range(each // SUB):
            for kk in range(owned):
                for m in range(parts):
                    row = (odd + 2 * SUB * t) * stride + kk * parts + m
                    out_ref[pl.ds(row, SUB, stride=2 * stride), :] = acc_ref[
                        pl.ds(odd * half + kk * each + t * SUB, SUB), pl.ds(m * LANES, LANES)
                    ]


def backward_x(msg_ref, ch_ref, cl_ref, out_ref, z_ref, y_ref, part_ref, sems, *, owned, group):
    depth, rows, width = out_ref.shape
    parts = rows // group
    half = width // 2
    each = half // owned
    stride = owned * parts
    for odd in range(2):
        for t in range(each // SUB):
            for kk in range(owned):
                for m in range(parts):
                    row = (odd + 2 * SUB * t) * stride + kk * parts + m
                    z_ref[pl.ds(odd * half + kk * each + t * SUB, SUB), pl.ds(m * LANES, LANES)] = msg_ref[
                        pl.ds(row, SUB, stride=2 * stride), :
                    ]
    for odd in range(2):
        at = pl.ds(odd * half, half)
        y_ref[odd] = dot3(split(z_ref[at, :].T), (ch_ref[at, :], cl_ref[at, :]), ((1,), (0,)))
    copies = []
    for m in range(parts):
        at = pl.ds(m * depth * group, depth * group)
        even, odd = y_ref[0, at, :], y_ref[1, at, :]
        near, far = even + odd, mirrored(even - odd)
        for z in range(depth):
            part_ref[z, pl.ds(m * group, group), pl.ds(0, half)] = near[z * group : z * group + group]
            part_ref[z, pl.ds(m * group, group), pl.ds(half, half)] = far[z * group : z * group + group]
        where = (slice(None), pl.ds(m * group, group), slice(None))
        copies.append(pltpu.make_async_copy(part_ref.at[where], out_ref.at[where], sems.at[m]))
        copies[-1].start()
    for copy in copies:
        copy.wait()


def coefficients(wid_in_ref, ek_ref, el_ref, cell_ref, link_ref, block_ref, wid_ref, red_ref, *, depth, tile):
    blocks = wid_in_ref.shape[0]
    owned, wide = ek_ref.shape[0], el_ref.shape[1]
    rows = depth * blocks
    cells = wide // LANES
    pitch = -(-owned * cells // SUB) * SUB

    wid_ref[...] = jnp.zeros(wid_ref.shape, jnp.float32)
    wid_ref[pl.ds(SUB, blocks), :] = wid_in_ref[...]
    width = wid_ref[pl.ds(SUB, blocks), :]
    before, after = wid_ref[pl.ds(SUB - 1, blocks), :], wid_ref[pl.ds(SUB + 1, blocks), :]
    column = lambda a, i: a[:, i : i + 1]
    width_of = [column(width, i) for i in range(depth)]
    padded = [column(before, depth - 1), *width_of, column(after, 0)]
    link = [2.0 / (padded[i] + padded[i + 1]) for i in range(depth + 1)]
    lower, upper = link[:-1], link[1:]
    red_ref[...] = jnp.zeros(red_ref.shape, jnp.float32)
    for i in range(depth):
        for index, value in ((0, upper[0] if i == 0 else lower[i]), (1, -upper[i])):
            link_ref[index, pl.ds(i * blocks, blocks), :] = jnp.broadcast_to(value / width_of[i], (blocks, LANES))

    def scatter(index, kk, t, value):
        for s in range(blocks // SUB):
            for c in range(tile // LANES):
                row = s * SUB * pitch + kk * cells + t * (tile // LANES) + c
                red_ref[index, pl.ds(row, SUB, stride=pitch), :] = value[
                    s * SUB : s * SUB + SUB, c * LANES : c * LANES + LANES
                ]

    for kk in range(owned):
        for t in range(wide // tile):
            cols = pl.ds(t * tile, tile)
            eigen = ek_ref[kk : kk + 1, :] + el_ref[:, cols]
            diagonal = lambda i: (lower[i] + upper[i]) + width_of[i] * eigen
            left, right = [None], [None]
            for i in range(1, depth):
                if i == 1:
                    inverse = 1.0 / diagonal(i)
                    left.append(-(inverse * lower[i]))
                else:
                    inverse = 1.0 / (diagonal(i) + lower[i] * right[-1])
                    left.append(inverse * lower[i] * left[-1])
                right.append(-(inverse * upper[i]))
                at = pl.ds(kk * rows + i * blocks, blocks)
                cell_ref[0, at, cols] = inverse * width_of[i]
                cell_ref[1, at, cols] = left[i]
            inner_left, inner_right = left[depth - 2], right[depth - 2]
            for i in range(depth - 3, 0, -1):
                inner_left = left[i] - right[i] * inner_left
                inner_right = -(right[i] * inner_right)
            inverse = 1.0 / (diagonal(0) + upper[0] * inner_left)
            at = pl.ds(kk * rows, blocks)
            cell_ref[0, at, cols] = inverse * width_of[0]
            cell_ref[1, at, cols] = jnp.zeros(inverse.shape, jnp.float32)
            scatter(0, kk, t, -(inverse * lower[0]))
            scatter(1, kk, t, inverse * upper[0] * inner_right)
            scatter(2, kk, t, left[depth - 1])
            scatter(3, kk, t, right[depth - 1])

    ratio = None
    for q in range(blocks):
        at = pl.ds(q * pitch, pitch)
        head_below, head_above, tail_below, tail_above = (red_ref[i, at, :] for i in range(4))
        if q == 0:
            head_own = jnp.ones(head_above.shape, jnp.float32)
            head_up = jnp.zeros(head_above.shape, jnp.float32)
            head_ratio = head_above
        else:
            head_own = 1.0 / (1.0 - head_below * ratio)
            head_up = -(head_below * head_own)
            head_ratio = head_above * head_own
        tail_own = 1.0 / (1.0 - tail_below * head_ratio)
        ratio = tail_above * tail_own
        found = (head_own, head_up, tail_own, -(tail_below * tail_own), head_ratio, ratio)
        for index, value in enumerate(found):
            block_ref[index, at, :] = value


def middle(
    msg_ref, sh_ref, sl_ref, cell_in, link_in, block_in, out_ref, a_ref, xh_ref, xl_ref, red_ref, cell_ref, link_ref,
    block_ref, sems, *, peers, blocks, depth, parts, group, owned, tile
):
    copies = start_copies(
        ((cell_in, cell_ref), (link_in, link_ref), (block_in, block_ref)), sems
    )
    wide = sh_ref.shape[1]
    stride = owned * parts
    halfs = peers // depth
    rows = depth * blocks
    cells = wide // LANES
    pitch = -(-owned * cells // SUB) * SUB

    def where(kk, zi):
        return pl.ds(kk * rows + zi * blocks, blocks)

    def slot(kk, m, g, h):
        return pl.ds((h * depth + g) * blocks * stride + kk * parts + m, blocks, stride=stride)

    def gather(m, h):
        got = [
            jnp.concatenate([msg_ref[slot(kk, m, g, h), :] for kk in range(owned)], 0) for g in range(depth)
        ]
        lanes = pl.ds((m * halfs + h) * LANES, LANES)
        for zi, block in enumerate(swap_groups(got, group)):
            high, low = split(block)
            for kk in range(owned):
                at = where(kk, zi)
                xh_ref[at, lanes] = high[kk * blocks : kk * blocks + blocks]
                xl_ref[at, lanes] = low[kk * blocks : kk * blocks + blocks]

    for m in range(parts):
        for h in range(halfs):
            gather(m, h)
        at = pl.ds(m * halfs * LANES, halfs * LANES)
        part = dot3((xh_ref[:, at], xl_ref[:, at]), (sh_ref[at, :], sl_ref[at, :]), ((1,), (0,)))
        if m == 0:
            a_ref[...] = part
        else:
            a_ref[...] += part
    for copy in copies:
        copy.wait()
    link = lambda index, i: jnp.concatenate([link_ref[index, pl.ds(i * blocks, blocks), :]] * (tile // LANES), 1)

    def scatter(index, kk, t, value):
        for s in range(blocks // SUB):
            for c in range(tile // LANES):
                row = s * SUB * pitch + kk * cells + t * (tile // LANES) + c
                red_ref[index, pl.ds(row, SUB, stride=pitch), :] = value[
                    s * SUB : s * SUB + SUB, c * LANES : c * LANES + LANES
                ]

    def reduce(kk):
        for t in range(wide // tile):
            cols = pl.ds(t * tile, tile)
            value = [None]
            for i in range(1, depth):
                at = where(kk, i)
                now = a_ref[at, cols]
                if i > 1:
                    now = now + link(0, i) * value[-1]
                value.append(cell_ref[0, at, cols] * now)
                if i < depth - 1:
                    a_ref[at, cols] = value[i]
            inner = value[depth - 2]
            for i in range(depth - 3, 0, -1):
                inner = value[i] - cell_ref[0, where(kk, i), cols] * (link(1, i) * inner)
            at = where(kk, 0)
            scatter(0, kk, t, cell_ref[0, at, cols] * (a_ref[at, cols] + link(0, 0) * inner))
            scatter(1, kk, t, value[depth - 1])

    red_ref[...] = jnp.zeros(red_ref.shape, jnp.float32)
    for kk in range(owned):
        reduce(kk)

    rhs = None
    for q in range(blocks):
        at = pl.ds(q * pitch, pitch)
        head = block_ref[0, at, :] * red_ref[0, at, :]
        if rhs is not None:
            head = head + block_ref[1, at, :] * rhs
        rhs = block_ref[2, at, :] * red_ref[1, at, :] + block_ref[3, at, :] * head
        red_ref[0, at, :] = head
        red_ref[1, at, :] = rhs
    following = None
    for q in range(blocks - 1, -1, -1):
        at = pl.ds(q * pitch, pitch)
        tail = red_ref[1, at, :]
        if following is not None:
            tail = tail - block_ref[5, at, :] * following
            red_ref[1, at, :] = tail
        following = red_ref[0, at, :] - block_ref[4, at, :] * tail
        red_ref[0, at, :] = following

    def column(index, kk, t):
        return jnp.concatenate(
            [
                jnp.concatenate(
                    [
                        red_ref[index, pl.ds(s * SUB * pitch + kk * cells + t * (tile // LANES) + c, SUB, stride=pitch), :]
                        for c in range(tile // LANES)
                    ],
                    1,
                )
                for s in range(blocks // SUB)
            ],
            0,
        )

    def substitute(kk):
        for t in range(wide // tile):
            cols = pl.ds(t * tile, tile)
            head, following = column(0, kk, t), column(1, kk, t)
            for zi, value in ((0, head), (depth - 1, following)):
                at = where(kk, zi)
                xh_ref[at, cols], xl_ref[at, cols] = split(value)
            for i in range(depth - 2, 0, -1):
                at = where(kk, i)
                free = a_ref[at, cols] - cell_ref[1, at, cols] * head
                following = free - cell_ref[0, at, cols] * (link(1, i) * following)
                xh_ref[at, cols], xl_ref[at, cols] = split(following)

    for kk in range(owned):
        substitute(kk)

    def send(m, h):
        lanes = pl.ds((m * halfs + h) * LANES, LANES)
        sent = swap_groups(
            [jnp.concatenate([a_ref[where(kk, zi), lanes] for kk in range(owned)], 0) for zi in range(depth)], group
        )
        for g, block in enumerate(sent):
            for kk in range(owned):
                out_ref[slot(kk, m, g, h), :] = block[kk * blocks : kk * blocks + blocks]

    for m in range(parts):
        at = pl.ds(m * halfs * LANES, halfs * LANES)
        a_ref[:, at] = dot3((xh_ref[...], xl_ref[...]), (sh_ref[:, at], sl_ref[:, at]), ((1,), (0,)))
        for h in range(halfs):
            send(m, h)


WHOLE = pl.BlockSpec(memory_space=VMEM)
PART = 256


def on_chip(*arrays):
    return [pltpu.with_memory_space_constraint(a, VMEM) for a in arrays]


def in_hbm(*arrays):
    return [pltpu.with_memory_space_constraint(a, pltpu.MemorySpace.HBM) for a in arrays]


HBM = pl.BlockSpec(memory_space=pltpu.MemorySpace.HBM)


def call_forward(source, high, low, owned, group):
    depth, rows, width = source.shape
    return pl.pallas_call(
        functools.partial(forward_x, owned=owned, group=group),
        name="forward_x",
        out_shape=pltpu.VMEM((width * depth * rows // LANES, LANES), jnp.float32),
        in_specs=[WHOLE, HBM, HBM],
        out_specs=WHOLE,
        scratch_shapes=[
            pltpu.VMEM((width, depth * rows), jnp.float32),
            pltpu.VMEM(high.shape, jnp.bfloat16),
            pltpu.VMEM(low.shape, jnp.bfloat16),
            pltpu.SemaphoreType.DMA((2,)),
        ],
    )(source, *in_hbm(high, low))


def call_backward(message, high, low, shape, owned, group):
    depth, rows, width = shape
    return pl.pallas_call(
        functools.partial(backward_x, owned=owned, group=group),
        name="backward_x",
        out_shape=jax.ShapeDtypeStruct(shape, jnp.float32),
        in_specs=[WHOLE] * 3,
        out_specs=HBM,
        scratch_shapes=[
            pltpu.VMEM((width, depth * rows), jnp.float32),
            pltpu.VMEM((2, depth * rows, width // 2), jnp.float32),
            pltpu.VMEM(shape, jnp.float32),
            pltpu.SemaphoreType.DMA((rows // group,)),
        ],
        compiler_params=pltpu.CompilerParams(vmem_limit_bytes=40 * 2**20),
    )(*on_chip(message, high, low))


def call_coefficients(widths, eigen_x, eigen_y, depth):
    blocks, owned, wide = widths.shape[0], eigen_x.shape[0], eigen_y.shape[1]
    pitch = -(-owned * (wide // LANES) // SUB) * SUB
    shapes = ((2, owned * depth * blocks, wide), (2, depth * blocks, LANES), (6, blocks * pitch, LANES))
    return pl.pallas_call(
        functools.partial(coefficients, depth=depth, tile=wide // 2),
        name="coefficients",
        out_shape=[jax.ShapeDtypeStruct(s, jnp.float32) for s in shapes],
        in_specs=[WHOLE] * 3,
        out_specs=[WHOLE] * 3,
        scratch_shapes=[
            pltpu.VMEM((blocks + 2 * SUB, LANES), jnp.float32),
            pltpu.VMEM((4, blocks * pitch, LANES), jnp.float32),
        ],
    )(widths, eigen_x, eigen_y)


def call_middle(message, high, low, cell, link, block, *, peers, blocks, depth, parts, group, owned):
    wide = high.shape[1]
    size = (owned * depth * blocks, wide)
    return pl.pallas_call(
        functools.partial(
            middle, peers=peers, blocks=blocks, depth=depth, parts=parts, group=group, owned=owned, tile=wide // 2
        ),
        name="middle",
        out_shape=pltpu.VMEM(message.shape, jnp.float32),
        in_specs=[WHOLE] * 3 + [HBM] * 3,
        out_specs=WHOLE,
        scratch_shapes=[
            pltpu.VMEM(size, jnp.float32),
            pltpu.VMEM(size, jnp.bfloat16),
            pltpu.VMEM(size, jnp.bfloat16),
            pltpu.VMEM((2, *block.shape[1:]), jnp.float32),
            pltpu.VMEM(cell.shape, jnp.float32),
            pltpu.VMEM(link.shape, jnp.float32),
            pltpu.VMEM(block.shape, jnp.float32),
            pltpu.SemaphoreType.DMA((3,)),
        ],
        compiler_params=pltpu.CompilerParams(vmem_limit_bytes=40 * 2**20),
    )(*on_chip(message, high, low), *in_hbm(cell, link, block))


def exchange(rows, devices):
    flat = rows.reshape(devices, 1, -1)
    return lax.all_to_all(flat, ALL, split_axis=0, concat_axis=0, tiled=True).reshape(-1, LANES)


def all_widths(cell_width, blocks):
    depth = cell_width.shape[0]
    row = lax.broadcasted_iota(jnp.int32, (blocks, LANES), 0)
    held = jnp.where(row == lax.axis_index("gz"), jnp.pad(cell_width, (0, LANES - depth))[None], 0.0)
    step = 1
    while step < blocks:
        held = held + lax.ppermute(held, "gz", [(i, i ^ step) for i in range(blocks)])
        step *= 2
    return held


def on_device(source, cell_width):
    depth, rows, width_x = source.shape
    peers, blocks = lax.axis_size("pa"), lax.axis_size("gz")
    devices = peers * blocks
    width_y = rows * peers
    owned = width_x // devices
    group = LANES // depth
    parts = rows // group

    cosines = halves(cosine_rows(width_x)[:, : width_x // 2].reshape(-1, 2, width_x // 2).swapaxes(0, 1).reshape(width_x, -1))
    order = order_y(np.arange(width_y), peers, parts, group)
    sines = sine_tables(peers, parts, group)
    got = exchange(call_forward(source, *cosines, owned, group), devices)

    own_k = jnp.arange(owned, dtype=jnp.int32) * devices + lax.axis_index(ALL)
    eigen_x, eigen_y = eigen_first(own_k, width_x)[:, None], eigen_second(jnp.asarray(order), width_y)[None]
    solve = call_coefficients(all_widths(cell_width, blocks), eigen_x, eigen_y, depth)
    back = call_middle(
        got, *sines, *solve,
        peers=peers, blocks=blocks, depth=depth, parts=parts, group=group, owned=owned,
    )
    return call_backward(exchange(back, devices), *cosines, source.shape, owned, group)


def solution(mesh):
    return jax.shard_map(
        on_device,
        mesh=mesh,
        in_specs=(P("gz", "pa", None), P("gz")),
        out_specs=P("gz", "pa", None),
        check_vma=False,
    )
```

```python
import functools
import math

import numpy as np

import jax
import jax.numpy as jnp
from jax import lax
from jax.experimental import pallas as pl
from jax.experimental.pallas import tpu as pltpu
from jax.sharding import PartitionSpec as P

ALL = ("pa", "gz")
LANES = 128
SUB = 8
VMEM = pltpu.MemorySpace.VMEM


def halves(table):
    table = table.astype(np.float32)
    high = table.astype(jnp.bfloat16)
    low = (table - high.astype(np.float32)).astype(jnp.bfloat16)
    return jnp.asarray(high), jnp.asarray(low)


def cosine_rows(width):
    k = np.arange(width)
    phases = k[:, None] * (2 * k[None, :] + 1) % (4 * width)
    weights = np.where(k == 0, math.sqrt(1.0 / width), math.sqrt(2.0 / width))
    return weights[:, None] * np.cos(phases * (math.pi / (2 * width)))


def order_y(values, peers, parts, group):
    return values.reshape(peers, parts, group).transpose(1, 0, 2).reshape(-1)


def sine_parts(peers, parts, group):
    width = peers * parts * group
    coarse = group * np.arange(peers * parts).reshape(peers, parts).T.reshape(-1)
    fine = np.arange(1, group + 1)
    cell = order_y(np.arange(1, width + 1), peers, parts, group)
    scale = math.sqrt(2.0 / (width + 1))

    def both(rows, scale):
        angle = rows[:, None] * cell[None] % (2 * (width + 1)) * (math.pi / (width + 1))
        return [jnp.asarray((scale * f(angle)).astype(np.float32)) for f in (np.sin, np.cos)]

    return both(coarse, scale) + both(fine, 1.0)


def sine_table(cs_ref, cc_ref, fs_ref, fc_ref, high_ref, low_ref):
    group = fs_ref.shape[0]

    def rows(i, _):
        here = pl.ds(i, 1)
        at = pl.ds(pl.multiple_of(i * group, group), group)
        high_ref[at, :], low_ref[at, :] = split(cs_ref[here, :] * fc_ref[...] + cc_ref[here, :] * fs_ref[...])
        return 0

    lax.fori_loop(0, cs_ref.shape[0], rows, 0)


def eigen_first(wavenumber, width):
    return 4.0 * jnp.square(jnp.sin(wavenumber.astype(jnp.float32) * (math.pi / (2 * width))))


def eigen_second(index, width):
    wavenumber = (index + 1).astype(jnp.float32)
    return 4.0 * jnp.square(jnp.sin(wavenumber * (math.pi / (2 * (width + 1)))))


def split(x):
    high = x.astype(jnp.bfloat16)
    return high, (x - high.astype(jnp.float32)).astype(jnp.bfloat16)


def dot3(a, b, dims):
    lhs = jnp.concatenate([a[0], a[1], a[0]], dims[0][0])
    rhs = jnp.concatenate([b[0], b[0], b[1]], dims[1][0])
    return lax.dot_general(lhs, rhs, (dims, ((), ())), preferred_element_type=jnp.float32)


def swap_groups(blocks, group):
    n = len(blocks)
    lanes = n * group
    lane = lax.broadcasted_iota(jnp.int32, blocks[0].shape, 1)
    blocks = list(blocks)
    d = 1
    while d < n:
        keep = (lane & (d * group)) == 0
        for i in range(n):
            if i & d:
                continue
            a, b = blocks[i], blocks[i + d]
            blocks[i] = jnp.where(keep, a, pltpu.roll(b, d * group, 1))
            blocks[i + d] = jnp.where(keep, pltpu.roll(a, lanes - d * group, 1), b)
        d *= 2
    return blocks


def mirrored(x):
    tiles = x.shape[1] // LANES
    lane = lax.broadcasted_iota(jnp.int32, (x.shape[0], LANES), 1)
    parts = [x[:, c * LANES : c * LANES + LANES] for c in range(tiles)]
    return jnp.concatenate([jnp.take_along_axis(p, LANES - 1 - lane, 1) for p in parts[::-1]], 1)


def start_copies(pairs, sems):
    copies = [pltpu.make_async_copy(a, b, sems.at[i]) for i, (a, b) in enumerate(pairs)]
    for copy in copies:
        copy.start()
    return copies


def forward_x(src_ref, ch_in, cl_in, out_ref, acc_ref, msg_ref, ch_ref, cl_ref, sems, *, owned, group):
    copies = start_copies(((ch_in, ch_ref), (cl_in, cl_ref)), sems)
    depth, rows, width = src_ref.shape
    parts = rows // group
    half = width // 2
    each = half // owned
    stride = owned * parts
    x = jnp.concatenate(
        [src_ref[z, pl.ds(m * group, group), :] for m in range(parts) for z in range(depth)], 0
    )
    near, far = x[:, :half], mirrored(x[:, half:])
    folded = split(near + far), split(near - far)
    for copy in copies:
        copy.wait()
    copies = []
    for odd in range(2):
        at = pl.ds(odd * half, half)
        acc_ref[at, :] = dot3((ch_ref[at, :], cl_ref[at, :]), folded[odd], ((1,), (1,)))
        for t in range(each // SUB):
            for kk in range(owned):
                for m in range(parts):
                    row = (odd * each + t * SUB) * stride + kk * parts + m
                    msg_ref[pl.ds(row, SUB, stride=stride), :] = acc_ref[
                        pl.ds(odd * half + kk * each + t * SUB, SUB), pl.ds(m * LANES, LANES)
                    ]
        at = pl.ds(odd * each * stride, each * stride)
        copies.append(pltpu.make_async_copy(msg_ref.at[at], out_ref.at[at], sems.at[2 + odd]))
        copies[-1].start()
    for copy in copies:
        copy.wait()


def backward_x(msg_ref, ch_ref, cl_ref, out_ref, z_ref, y_ref, part_ref, sems, *, owned, group):
    depth, rows, width = out_ref.shape
    parts = rows // group
    half = width // 2
    each = half // owned
    stride = owned * parts
    for odd in range(2):
        for t in range(each // SUB):
            for kk in range(owned):
                for m in range(parts):
                    row = (odd * each + t * SUB) * stride + kk * parts + m
                    z_ref[pl.ds(odd * half + kk * each + t * SUB, SUB), pl.ds(m * LANES, LANES)] = msg_ref[
                        pl.ds(row, SUB, stride=stride), :
                    ]
    for odd in range(2):
        at = pl.ds(odd * half, half)
        y_ref[odd] = dot3(split(z_ref[at, :].T), (ch_ref[at, :], cl_ref[at, :]), ((1,), (0,)))
    copies = []
    for m in range(parts):
        at = pl.ds(m * depth * group, depth * group)
        even, odd = y_ref[0, at, :], y_ref[1, at, :]
        near, far = even + odd, mirrored(even - odd)
        for z in range(depth):
            part_ref[z, pl.ds(m * group, group), pl.ds(0, half)] = near[z * group : z * group + group]
            part_ref[z, pl.ds(m * group, group), pl.ds(half, half)] = far[z * group : z * group + group]
        where = (slice(None), pl.ds(m * group, group), slice(None))
        copies.append(pltpu.make_async_copy(part_ref.at[where], out_ref.at[where], sems.at[m]))
        copies[-1].start()
    for copy in copies:
        copy.wait()


def coefficients(wid_in_ref, ek_ref, el_ref, cell_ref, link_ref, block_ref, wid_ref, red_ref, *, depth, tile):
    blocks = wid_in_ref.shape[0]
    owned, wide = ek_ref.shape[0], el_ref.shape[1]
    rows = depth * blocks
    cells = wide // LANES
    pitch = -(-owned * cells // SUB) * SUB

    wid_ref[...] = jnp.zeros(wid_ref.shape, jnp.float32)
    wid_ref[pl.ds(SUB, blocks), :] = wid_in_ref[...]
    width = wid_ref[pl.ds(SUB, blocks), :]
    before, after = wid_ref[pl.ds(SUB - 1, blocks), :], wid_ref[pl.ds(SUB + 1, blocks), :]
    column = lambda a, i: a[:, i : i + 1]
    width_of = [column(width, i) for i in range(depth)]
    padded = [column(before, depth - 1), *width_of, column(after, 0)]
    link = [2.0 / (padded[i] + padded[i + 1]) for i in range(depth + 1)]
    lower, upper = link[:-1], link[1:]
    red_ref[...] = jnp.zeros(red_ref.shape, jnp.float32)
    for i in range(depth):
        for index, value in ((0, upper[0] if i == 0 else lower[i]), (1, -upper[i])):
            link_ref[index, pl.ds(i * blocks, blocks), :] = jnp.broadcast_to(value / width_of[i], (blocks, LANES))

    def scatter(index, kk, t, value):
        for s in range(blocks // SUB):
            for c in range(tile // LANES):
                row = s * SUB * pitch + kk * cells + t * (tile // LANES) + c
                red_ref[index, pl.ds(row, SUB, stride=pitch), :] = value[
                    s * SUB : s * SUB + SUB, c * LANES : c * LANES + LANES
                ]

    for kk in range(owned):
        for t in range(wide // tile):
            cols = pl.ds(t * tile, tile)
            eigen = ek_ref[kk : kk + 1, :] + el_ref[:, cols]
            diagonal = lambda i: (lower[i] + upper[i]) + width_of[i] * eigen
            left, right = [None], [None]
            for i in range(1, depth):
                if i == 1:
                    inverse = 1.0 / diagonal(i)
                    left.append(-(inverse * lower[i]))
                else:
                    inverse = 1.0 / (diagonal(i) + lower[i] * right[-1])
                    left.append(inverse * lower[i] * left[-1])
                right.append(-(inverse * upper[i]))
                at = pl.ds(kk * rows + i * blocks, blocks)
                cell_ref[0, at, cols] = inverse * width_of[i]
                cell_ref[1, at, cols] = left[i]
            inner_left, inner_right = left[depth - 2], right[depth - 2]
            for i in range(depth - 3, 0, -1):
                inner_left = left[i] - right[i] * inner_left
                inner_right = -(right[i] * inner_right)
            inverse = 1.0 / (diagonal(0) + upper[0] * inner_left)
            at = pl.ds(kk * rows, blocks)
            cell_ref[0, at, cols] = inverse * width_of[0]
            cell_ref[1, at, cols] = jnp.zeros(inverse.shape, jnp.float32)
            scatter(0, kk, t, -(inverse * lower[0]))
            scatter(1, kk, t, inverse * upper[0] * inner_right)
            scatter(2, kk, t, left[depth - 1])
            scatter(3, kk, t, right[depth - 1])

    ratio = None
    for q in range(blocks):
        at = pl.ds(q * pitch, pitch)
        head_below, head_above, tail_below, tail_above = (red_ref[i, at, :] for i in range(4))
        if q == 0:
            head_own = jnp.ones(head_above.shape, jnp.float32)
            head_up = jnp.zeros(head_above.shape, jnp.float32)
            head_ratio = head_above
        else:
            head_own = 1.0 / (1.0 - head_below * ratio)
            head_up = -(head_below * head_own)
            head_ratio = head_above * head_own
        tail_own = 1.0 / (1.0 - tail_below * head_ratio)
        ratio = tail_above * tail_own
        found = (head_own, head_up, tail_own, -(tail_below * tail_own), head_ratio, ratio)
        for index, value in enumerate(found):
            block_ref[index, at, :] = value


def middle(
    msg_ref, sh_ref, sl_ref, cell_in, link_in, block_in, out_ref, a_ref, xh_ref, xl_ref, red_ref, cell_ref, link_ref,
    block_ref, sems, *, peers, blocks, depth, parts, group, owned, tile
):
    copies = start_copies(
        ((cell_in, cell_ref), (link_in, link_ref), (block_in, block_ref)), sems
    )
    wide = sh_ref.shape[1]
    stride = owned * parts
    halfs = peers // depth
    rows = depth * blocks
    cells = wide // LANES
    pitch = -(-owned * cells // SUB) * SUB

    def where(kk, zi):
        return pl.ds(kk * rows + zi * blocks, blocks)

    def slot(kk, m, g, h):
        return pl.ds((h * depth + g) * blocks * stride + kk * parts + m, blocks, stride=stride)

    def gather(m, h):
        got = [
            jnp.concatenate([msg_ref[slot(kk, m, g, h), :] for kk in range(owned)], 0) for g in range(depth)
        ]
        lanes = pl.ds((m * halfs + h) * LANES, LANES)
        for zi, block in enumerate(swap_groups(got, group)):
            high, low = split(block)
            for kk in range(owned):
                at = where(kk, zi)
                xh_ref[at, lanes] = high[kk * blocks : kk * blocks + blocks]
                xl_ref[at, lanes] = low[kk * blocks : kk * blocks + blocks]

    for m in range(parts):
        for h in range(halfs):
            gather(m, h)
        at = pl.ds(m * halfs * LANES, halfs * LANES)
        part = dot3((xh_ref[:, at], xl_ref[:, at]), (sh_ref[at, :], sl_ref[at, :]), ((1,), (0,)))
        if m == 0:
            a_ref[...] = part
        else:
            a_ref[...] += part
    for copy in copies:
        copy.wait()
    link = lambda index, i: jnp.concatenate([link_ref[index, pl.ds(i * blocks, blocks), :]] * (tile // LANES), 1)

    def scatter(index, kk, t, value):
        for s in range(blocks // SUB):
            for c in range(tile // LANES):
                row = s * SUB * pitch + kk * cells + t * (tile // LANES) + c
                red_ref[index, pl.ds(row, SUB, stride=pitch), :] = value[
                    s * SUB : s * SUB + SUB, c * LANES : c * LANES + LANES
                ]

    def reduce(kk):
        for t in range(wide // tile):
            cols = pl.ds(t * tile, tile)
            value = [None]
            for i in range(1, depth):
                at = where(kk, i)
                now = a_ref[at, cols]
                if i > 1:
                    now = now + link(0, i) * value[-1]
                value.append(cell_ref[0, at, cols] * now)
                if i < depth - 1:
                    a_ref[at, cols] = value[i]
            inner = value[depth - 2]
            for i in range(depth - 3, 0, -1):
                inner = value[i] - cell_ref[0, where(kk, i), cols] * (link(1, i) * inner)
            at = where(kk, 0)
            scatter(0, kk, t, cell_ref[0, at, cols] * (a_ref[at, cols] + link(0, 0) * inner))
            scatter(1, kk, t, value[depth - 1])

    red_ref[...] = jnp.zeros(red_ref.shape, jnp.float32)
    for kk in range(owned):
        reduce(kk)

    rhs = None
    for q in range(blocks):
        at = pl.ds(q * pitch, pitch)
        head = block_ref[0, at, :] * red_ref[0, at, :]
        if rhs is not None:
            head = head + block_ref[1, at, :] * rhs
        rhs = block_ref[2, at, :] * red_ref[1, at, :] + block_ref[3, at, :] * head
        red_ref[0, at, :] = head
        red_ref[1, at, :] = rhs
    following = None
    for q in range(blocks - 1, -1, -1):
        at = pl.ds(q * pitch, pitch)
        tail = red_ref[1, at, :]
        if following is not None:
            tail = tail - block_ref[5, at, :] * following
            red_ref[1, at, :] = tail
        following = red_ref[0, at, :] - block_ref[4, at, :] * tail
        red_ref[0, at, :] = following

    def column(index, kk, t):
        return jnp.concatenate(
            [
                jnp.concatenate(
                    [
                        red_ref[index, pl.ds(s * SUB * pitch + kk * cells + t * (tile // LANES) + c, SUB, stride=pitch), :]
                        for c in range(tile // LANES)
                    ],
                    1,
                )
                for s in range(blocks // SUB)
            ],
            0,
        )

    def substitute(kk):
        for t in range(wide // tile):
            cols = pl.ds(t * tile, tile)
            head, following = column(0, kk, t), column(1, kk, t)
            for zi, value in ((0, head), (depth - 1, following)):
                at = where(kk, zi)
                xh_ref[at, cols], xl_ref[at, cols] = split(value)
            for i in range(depth - 2, 0, -1):
                at = where(kk, i)
                free = a_ref[at, cols] - cell_ref[1, at, cols] * head
                following = free - cell_ref[0, at, cols] * (link(1, i) * following)
                xh_ref[at, cols], xl_ref[at, cols] = split(following)

    for kk in range(owned):
        substitute(kk)

    def send(m, h):
        lanes = pl.ds((m * halfs + h) * LANES, LANES)
        sent = swap_groups(
            [jnp.concatenate([a_ref[where(kk, zi), lanes] for kk in range(owned)], 0) for zi in range(depth)], group
        )
        for g, block in enumerate(sent):
            for kk in range(owned):
                out_ref[slot(kk, m, g, h), :] = block[kk * blocks : kk * blocks + blocks]

    for m in range(parts):
        at = pl.ds(m * halfs * LANES, halfs * LANES)
        a_ref[:, at] = dot3((xh_ref[...], xl_ref[...]), (sh_ref[:, at], sl_ref[:, at]), ((1,), (0,)))
        for h in range(halfs):
            send(m, h)


WHOLE = pl.BlockSpec(memory_space=VMEM)
PART = 256


def on_chip(*arrays):
    return [pltpu.with_memory_space_constraint(a, VMEM) for a in arrays]


def in_hbm(*arrays):
    return [pltpu.with_memory_space_constraint(a, pltpu.MemorySpace.HBM) for a in arrays]


HBM = pl.BlockSpec(memory_space=pltpu.MemorySpace.HBM)


def call_forward(source, high, low, owned, group):
    depth, rows, width = source.shape
    return pl.pallas_call(
        functools.partial(forward_x, owned=owned, group=group),
        name="forward_x",
        out_shape=jax.ShapeDtypeStruct((width * depth * rows // LANES, LANES), jnp.float32),
        in_specs=[WHOLE, HBM, HBM],
        out_specs=HBM,
        scratch_shapes=[
            pltpu.VMEM((width, depth * rows), jnp.float32),
            pltpu.VMEM((width * depth * rows // LANES, LANES), jnp.float32),
            pltpu.VMEM(high.shape, jnp.bfloat16),
            pltpu.VMEM(low.shape, jnp.bfloat16),
            pltpu.SemaphoreType.DMA((4,)),
        ],
    )(source, *in_hbm(high, low))


def call_backward(message, high, low, shape, owned, group):
    depth, rows, width = shape
    return pl.pallas_call(
        functools.partial(backward_x, owned=owned, group=group),
        name="backward_x",
        out_shape=jax.ShapeDtypeStruct(shape, jnp.float32),
        in_specs=[WHOLE] * 3,
        out_specs=HBM,
        scratch_shapes=[
            pltpu.VMEM((width, depth * rows), jnp.float32),
            pltpu.VMEM((2, depth * rows, width // 2), jnp.float32),
            pltpu.VMEM(shape, jnp.float32),
            pltpu.SemaphoreType.DMA((rows // group,)),
        ],
        compiler_params=pltpu.CompilerParams(vmem_limit_bytes=40 * 2**20),
    )(*on_chip(message, high, low))


def sine_tables(peers, parts, group):
    width = peers * parts * group
    return pl.pallas_call(
        sine_table,
        name="sine_table",
        out_shape=[pltpu.VMEM((width, width), jnp.bfloat16)] * 2,
        in_specs=[WHOLE] * 4,
        out_specs=[WHOLE] * 2,
    )(*sine_parts(peers, parts, group))


def call_coefficients(widths, eigen_x, eigen_y, depth):
    blocks, owned, wide = widths.shape[0], eigen_x.shape[0], eigen_y.shape[1]
    pitch = -(-owned * (wide // LANES) // SUB) * SUB
    shapes = ((2, owned * depth * blocks, wide), (2, depth * blocks, LANES), (6, blocks * pitch, LANES))
    return pl.pallas_call(
        functools.partial(coefficients, depth=depth, tile=wide // 2),
        name="coefficients",
        out_shape=[jax.ShapeDtypeStruct(s, jnp.float32) for s in shapes],
        in_specs=[WHOLE] * 3,
        out_specs=[WHOLE] * 3,
        scratch_shapes=[
            pltpu.VMEM((blocks + 2 * SUB, LANES), jnp.float32),
            pltpu.VMEM((4, blocks * pitch, LANES), jnp.float32),
        ],
    )(widths, eigen_x, eigen_y)


def call_middle(message, high, low, cell, link, block, *, peers, blocks, depth, parts, group, owned):
    wide = high.shape[1]
    size = (owned * depth * blocks, wide)
    return pl.pallas_call(
        functools.partial(
            middle, peers=peers, blocks=blocks, depth=depth, parts=parts, group=group, owned=owned, tile=wide // 2
        ),
        name="middle",
        out_shape=pltpu.VMEM(message.shape, jnp.float32),
        in_specs=[WHOLE] * 3 + [HBM] * 3,
        out_specs=WHOLE,
        scratch_shapes=[
            pltpu.VMEM(size, jnp.float32),
            pltpu.VMEM(size, jnp.bfloat16),
            pltpu.VMEM(size, jnp.bfloat16),
            pltpu.VMEM((2, *block.shape[1:]), jnp.float32),
            pltpu.VMEM(cell.shape, jnp.float32),
            pltpu.VMEM(link.shape, jnp.float32),
            pltpu.VMEM(block.shape, jnp.float32),
            pltpu.SemaphoreType.DMA((3,)),
        ],
        compiler_params=pltpu.CompilerParams(vmem_limit_bytes=40 * 2**20),
    )(*on_chip(message, high, low), *in_hbm(cell, link, block))


def exchange(rows, devices):
    flat = rows.reshape(devices, 1, -1)
    return lax.all_to_all(flat, ALL, split_axis=0, concat_axis=0, tiled=True).reshape(-1, LANES)


def all_widths(cell_width, blocks):
    depth = cell_width.shape[0]
    row = lax.broadcasted_iota(jnp.int32, (blocks, LANES), 0)
    held = jnp.where(row == lax.axis_index("gz"), jnp.pad(cell_width, (0, LANES - depth))[None], 0.0)
    step = 1
    while step < blocks:
        held = held + lax.ppermute(held, "gz", [(i, i ^ step) for i in range(blocks)])
        step *= 2
    return held


def on_device(source, cell_width):
    depth, rows, width_x = source.shape
    peers, blocks = lax.axis_size("pa"), lax.axis_size("gz")
    devices = peers * blocks
    width_y = rows * peers
    owned = width_x // devices
    group = LANES // depth
    parts = rows // group

    cosines = halves(cosine_rows(width_x)[:, : width_x // 2].reshape(-1, 2, width_x // 2).swapaxes(0, 1).reshape(width_x, -1))
    order = order_y(np.arange(width_y), peers, parts, group)
    sines = sine_tables(peers, parts, group)
    got = exchange(call_forward(source, *cosines, owned, group), devices)

    device, half = lax.axis_index(ALL), devices // 2
    own_k = 2 * (jnp.arange(owned, dtype=jnp.int32) * half + device % half) + device // half
    eigen_x, eigen_y = eigen_first(own_k, width_x)[:, None], eigen_second(jnp.asarray(order), width_y)[None]
    solve = call_coefficients(all_widths(cell_width, blocks), eigen_x, eigen_y, depth)
    back = call_middle(
        got, *sines, *solve,
        peers=peers, blocks=blocks, depth=depth, parts=parts, group=group, owned=owned,
    )
    return call_backward(exchange(back, devices), *cosines, source.shape, owned, group)


def solution(mesh):
    return jax.shard_map(
        on_device,
        mesh=mesh,
        in_specs=(P("gz", "pa", None), P("gz")),
        out_specs=P("gz", "pa", None),
        check_vma=False,
    )
```

```python
import functools
import math

import numpy as np

import jax
import jax.numpy as jnp
from jax import lax
from jax.experimental import pallas as pl
from jax.experimental.pallas import tpu as pltpu
from jax.sharding import PartitionSpec as P

ALL = ("pa", "gz")
LANES = 128
SUB = 8
VMEM = pltpu.MemorySpace.VMEM


def halves(table):
    table = table.astype(np.float32)
    high = table.astype(jnp.bfloat16)
    low = (table - high.astype(np.float32)).astype(jnp.bfloat16)
    return jnp.asarray(high), jnp.asarray(low)


def cosine_rows(width):
    k = np.arange(width)
    phases = k[:, None] * (2 * k[None, :] + 1) % (4 * width)
    weights = np.where(k == 0, math.sqrt(1.0 / width), math.sqrt(2.0 / width))
    return weights[:, None] * np.cos(phases * (math.pi / (2 * width)))


def order_y(values, peers, parts, group):
    return values.reshape(peers, parts, group).transpose(1, 0, 2).reshape(-1)


def sine_parts(peers, parts, group):
    width = peers * parts * group
    coarse = group * np.arange(peers * parts).reshape(peers, parts).T.reshape(-1)
    fine = np.arange(1, group + 1)
    cell = order_y(np.arange(1, width + 1), peers, parts, group)
    scale = math.sqrt(2.0 / (width + 1))

    def both(rows, scale):
        angle = rows[:, None] * cell[None] % (2 * (width + 1)) * (math.pi / (width + 1))
        return [jnp.asarray((scale * f(angle)).astype(np.float32)) for f in (np.sin, np.cos)]

    return both(coarse, scale) + both(fine, 1.0)


def sine_table(cs_ref, cc_ref, fs_ref, fc_ref, high_ref, low_ref):
    group = fs_ref.shape[0]

    def rows(i, _):
        here = pl.ds(i, 1)
        at = pl.ds(pl.multiple_of(i * group, group), group)
        high_ref[at, :], low_ref[at, :] = split(cs_ref[here, :] * fc_ref[...] + cc_ref[here, :] * fs_ref[...])
        return 0

    lax.fori_loop(0, cs_ref.shape[0], rows, 0)


def eigen_first(wavenumber, width):
    return 4.0 * jnp.square(jnp.sin(wavenumber.astype(jnp.float32) * (math.pi / (2 * width))))


def eigen_second(index, width):
    wavenumber = (index + 1).astype(jnp.float32)
    return 4.0 * jnp.square(jnp.sin(wavenumber * (math.pi / (2 * (width + 1)))))


def split(x):
    high = x.astype(jnp.bfloat16)
    return high, (x - high.astype(jnp.float32)).astype(jnp.bfloat16)


def dot3(a, b, dims):
    lhs = jnp.concatenate([a[0], a[1], a[0]], dims[0][0])
    rhs = jnp.concatenate([b[0], b[0], b[1]], dims[1][0])
    return lax.dot_general(lhs, rhs, (dims, ((), ())), preferred_element_type=jnp.float32)


def swap_groups(blocks, group):
    n = len(blocks)
    lanes = n * group
    lane = lax.broadcasted_iota(jnp.int32, blocks[0].shape, 1)
    blocks = list(blocks)
    d = 1
    while d < n:
        keep = (lane & (d * group)) == 0
        for i in range(n):
            if i & d:
                continue
            a, b = blocks[i], blocks[i + d]
            blocks[i] = jnp.where(keep, a, pltpu.roll(b, d * group, 1))
            blocks[i + d] = jnp.where(keep, pltpu.roll(a, lanes - d * group, 1), b)
        d *= 2
    return blocks


def mirrored(x):
    tiles = x.shape[1] // LANES
    lane = lax.broadcasted_iota(jnp.int32, (x.shape[0], LANES), 1)
    parts = [x[:, c * LANES : c * LANES + LANES] for c in range(tiles)]
    return jnp.concatenate([jnp.take_along_axis(p, LANES - 1 - lane, 1) for p in parts[::-1]], 1)


def start_copies(pairs, sems):
    copies = [pltpu.make_async_copy(a, b, sems.at[i]) for i, (a, b) in enumerate(pairs)]
    for copy in copies:
        copy.start()
    return copies


def forward_x(
    src_in, ch_in, cl_in, out_ref, src_ref, xh_ref, xl_ref, acc_ref, msg_ref, ch_ref, cl_ref, sems, *, owned, group
):
    depth, rows, width = src_in.shape
    parts = rows // group
    pieces = [(slice(None), pl.ds(m * group, group), slice(None)) for m in range(parts)]
    copies = start_copies(
        [(src_in.at[piece], src_ref.at[piece]) for piece in pieces] + [(ch_in, ch_ref), (cl_in, cl_ref)], sems
    )
    half = width // 2
    each = half // owned
    stride = owned * parts
    for m in range(parts):
        copies[m].wait()
        x = jnp.concatenate([src_ref[z, pl.ds(m * group, group), :] for z in range(depth)], 0)
        near, far = x[:, :half], mirrored(x[:, half:])
        at = pl.ds(m * depth * group, depth * group)
        for odd, folded in enumerate((near + far, near - far)):
            xh_ref[odd, at, :], xl_ref[odd, at, :] = split(folded)
    for copy in copies[parts:]:
        copy.wait()
    copies = []
    for odd in range(2):
        at = pl.ds(odd * half, half)
        acc_ref[at, :] = dot3((ch_ref[at, :], cl_ref[at, :]), (xh_ref[odd], xl_ref[odd]), ((1,), (1,)))
        for t in range(each // SUB):
            for kk in range(owned):
                for m in range(parts):
                    row = (odd * each + t * SUB) * stride + kk * parts + m
                    msg_ref[pl.ds(row, SUB, stride=stride), :] = acc_ref[
                        pl.ds(odd * half + kk * each + t * SUB, SUB), pl.ds(m * LANES, LANES)
                    ]
        at = pl.ds(odd * each * stride, each * stride)
        copies.append(pltpu.make_async_copy(msg_ref.at[at], out_ref.at[at], sems.at[parts + 2 + odd]))
        copies[-1].start()
    for copy in copies:
        copy.wait()


def backward_x(msg_ref, ch_ref, cl_ref, out_ref, z_ref, y_ref, part_ref, sems, *, owned, group):
    depth, rows, width = out_ref.shape
    parts = rows // group
    half = width // 2
    each = half // owned
    stride = owned * parts
    for odd in range(2):
        for t in range(each // SUB):
            for kk in range(owned):
                for m in range(parts):
                    row = (odd * each + t * SUB) * stride + kk * parts + m
                    z_ref[pl.ds(odd * half + kk * each + t * SUB, SUB), pl.ds(m * LANES, LANES)] = msg_ref[
                        pl.ds(row, SUB, stride=stride), :
                    ]
    for odd in range(2):
        at = pl.ds(odd * half, half)
        y_ref[odd] = dot3(split(z_ref[at, :].T), (ch_ref[at, :], cl_ref[at, :]), ((1,), (0,)))
    copies = []
    for m in range(parts):
        at = pl.ds(m * depth * group, depth * group)
        even, odd = y_ref[0, at, :], y_ref[1, at, :]
        near, far = even + odd, mirrored(even - odd)
        for z in range(depth):
            part_ref[z, pl.ds(m * group, group), pl.ds(0, half)] = near[z * group : z * group + group]
            part_ref[z, pl.ds(m * group, group), pl.ds(half, half)] = far[z * group : z * group + group]
        where = (slice(None), pl.ds(m * group, group), slice(None))
        copies.append(pltpu.make_async_copy(part_ref.at[where], out_ref.at[where], sems.at[m]))
        copies[-1].start()
    for copy in copies:
        copy.wait()


def coefficients(wid_in_ref, ek_ref, el_ref, cell_ref, link_ref, block_ref, wid_ref, red_ref, *, depth, tile):
    blocks = wid_in_ref.shape[0]
    owned, wide = ek_ref.shape[0], el_ref.shape[1]
    rows = depth * blocks
    cells = wide // LANES
    pitch = -(-owned * cells // SUB) * SUB

    wid_ref[...] = jnp.zeros(wid_ref.shape, jnp.float32)
    wid_ref[pl.ds(SUB, blocks), :] = wid_in_ref[...]
    width = wid_ref[pl.ds(SUB, blocks), :]
    before, after = wid_ref[pl.ds(SUB - 1, blocks), :], wid_ref[pl.ds(SUB + 1, blocks), :]
    column = lambda a, i: a[:, i : i + 1]
    width_of = [column(width, i) for i in range(depth)]
    padded = [column(before, depth - 1), *width_of, column(after, 0)]
    link = [2.0 / (padded[i] + padded[i + 1]) for i in range(depth + 1)]
    lower, upper = link[:-1], link[1:]
    red_ref[...] = jnp.zeros(red_ref.shape, jnp.float32)
    for i in range(depth):
        for index, value in ((0, upper[0] if i == 0 else lower[i]), (1, -upper[i])):
            link_ref[index, pl.ds(i * blocks, blocks), :] = jnp.broadcast_to(value / width_of[i], (blocks, LANES))

    def scatter(index, kk, t, value):
        for s in range(blocks // SUB):
            for c in range(tile // LANES):
                row = s * SUB * pitch + kk * cells + t * (tile // LANES) + c
                red_ref[index, pl.ds(row, SUB, stride=pitch), :] = value[
                    s * SUB : s * SUB + SUB, c * LANES : c * LANES + LANES
                ]

    for kk in range(owned):
        for t in range(wide // tile):
            cols = pl.ds(t * tile, tile)
            eigen = ek_ref[kk : kk + 1, :] + el_ref[:, cols]
            diagonal = lambda i: (lower[i] + upper[i]) + width_of[i] * eigen
            left, right = [None], [None]
            for i in range(1, depth):
                if i == 1:
                    inverse = 1.0 / diagonal(i)
                    left.append(-(inverse * lower[i]))
                else:
                    inverse = 1.0 / (diagonal(i) + lower[i] * right[-1])
                    left.append(inverse * lower[i] * left[-1])
                right.append(-(inverse * upper[i]))
                at = pl.ds(kk * rows + i * blocks, blocks)
                cell_ref[0, at, cols] = inverse * width_of[i]
                cell_ref[1, at, cols] = left[i]
            inner_left, inner_right = left[depth - 2], right[depth - 2]
            for i in range(depth - 3, 0, -1):
                inner_left = left[i] - right[i] * inner_left
                inner_right = -(right[i] * inner_right)
            inverse = 1.0 / (diagonal(0) + upper[0] * inner_left)
            at = pl.ds(kk * rows, blocks)
            cell_ref[0, at, cols] = inverse * width_of[0]
            cell_ref[1, at, cols] = jnp.zeros(inverse.shape, jnp.float32)
            scatter(0, kk, t, -(inverse * lower[0]))
            scatter(1, kk, t, inverse * upper[0] * inner_right)
            scatter(2, kk, t, left[depth - 1])
            scatter(3, kk, t, right[depth - 1])

    ratio = None
    for q in range(blocks):
        at = pl.ds(q * pitch, pitch)
        head_below, head_above, tail_below, tail_above = (red_ref[i, at, :] for i in range(4))
        if q == 0:
            head_own = jnp.ones(head_above.shape, jnp.float32)
            head_up = jnp.zeros(head_above.shape, jnp.float32)
            head_ratio = head_above
        else:
            head_own = 1.0 / (1.0 - head_below * ratio)
            head_up = -(head_below * head_own)
            head_ratio = head_above * head_own
        tail_own = 1.0 / (1.0 - tail_below * head_ratio)
        ratio = tail_above * tail_own
        found = (head_own, head_up, tail_own, -(tail_below * tail_own), head_ratio, ratio)
        for index, value in enumerate(found):
            block_ref[index, at, :] = value


def middle(
    msg_ref, sh_ref, sl_ref, cell_in, link_in, block_in, out_ref, a_ref, xh_ref, xl_ref, red_ref, cell_ref, link_ref,
    block_ref, sems, *, peers, blocks, depth, parts, group, owned, tile
):
    copies = start_copies(
        ((cell_in, cell_ref), (link_in, link_ref), (block_in, block_ref)), sems
    )
    wide = sh_ref.shape[1]
    stride = owned * parts
    halfs = peers // depth
    rows = depth * blocks
    cells = wide // LANES
    pitch = -(-owned * cells // SUB) * SUB

    def where(kk, zi):
        return pl.ds(kk * rows + zi * blocks, blocks)

    def slot(kk, m, g, h):
        return pl.ds((h * depth + g) * blocks * stride + kk * parts + m, blocks, stride=stride)

    def gather(m, h):
        got = [
            jnp.concatenate([msg_ref[slot(kk, m, g, h), :] for kk in range(owned)], 0) for g in range(depth)
        ]
        lanes = pl.ds((m * halfs + h) * LANES, LANES)
        for zi, block in enumerate(swap_groups(got, group)):
            high, low = split(block)
            for kk in range(owned):
                at = where(kk, zi)
                xh_ref[at, lanes] = high[kk * blocks : kk * blocks + blocks]
                xl_ref[at, lanes] = low[kk * blocks : kk * blocks + blocks]

    for m in range(parts):
        for h in range(halfs):
            gather(m, h)
        at = pl.ds(m * halfs * LANES, halfs * LANES)
        part = dot3((xh_ref[:, at], xl_ref[:, at]), (sh_ref[at, :], sl_ref[at, :]), ((1,), (0,)))
        if m == 0:
            a_ref[...] = part
        else:
            a_ref[...] += part
    for copy in copies:
        copy.wait()
    link = lambda index, i: jnp.concatenate([link_ref[index, pl.ds(i * blocks, blocks), :]] * (tile // LANES), 1)

    def scatter(index, kk, t, value):
        for s in range(blocks // SUB):
            for c in range(tile // LANES):
                row = s * SUB * pitch + kk * cells + t * (tile // LANES) + c
                red_ref[index, pl.ds(row, SUB, stride=pitch), :] = value[
                    s * SUB : s * SUB + SUB, c * LANES : c * LANES + LANES
                ]

    def reduce(kk):
        for t in range(wide // tile):
            cols = pl.ds(t * tile, tile)
            value = [None]
            for i in range(1, depth):
                at = where(kk, i)
                now = a_ref[at, cols]
                if i > 1:
                    now = now + link(0, i) * value[-1]
                value.append(cell_ref[0, at, cols] * now)
                if i < depth - 1:
                    a_ref[at, cols] = value[i]
            inner = value[depth - 2]
            for i in range(depth - 3, 0, -1):
                inner = value[i] - cell_ref[0, where(kk, i), cols] * (link(1, i) * inner)
            at = where(kk, 0)
            scatter(0, kk, t, cell_ref[0, at, cols] * (a_ref[at, cols] + link(0, 0) * inner))
            scatter(1, kk, t, value[depth - 1])

    red_ref[...] = jnp.zeros(red_ref.shape, jnp.float32)
    for kk in range(owned):
        reduce(kk)

    rhs = None
    for q in range(blocks):
        at = pl.ds(q * pitch, pitch)
        head = block_ref[0, at, :] * red_ref[0, at, :]
        if rhs is not None:
            head = head + block_ref[1, at, :] * rhs
        rhs = block_ref[2, at, :] * red_ref[1, at, :] + block_ref[3, at, :] * head
        red_ref[0, at, :] = head
        red_ref[1, at, :] = rhs
    following = None
    for q in range(blocks - 1, -1, -1):
        at = pl.ds(q * pitch, pitch)
        tail = red_ref[1, at, :]
        if following is not None:
            tail = tail - block_ref[5, at, :] * following
            red_ref[1, at, :] = tail
        following = red_ref[0, at, :] - block_ref[4, at, :] * tail
        red_ref[0, at, :] = following

    def column(index, kk, t):
        return jnp.concatenate(
            [
                jnp.concatenate(
                    [
                        red_ref[index, pl.ds(s * SUB * pitch + kk * cells + t * (tile // LANES) + c, SUB, stride=pitch), :]
                        for c in range(tile // LANES)
                    ],
                    1,
                )
                for s in range(blocks // SUB)
            ],
            0,
        )

    def substitute(kk):
        for t in range(wide // tile):
            cols = pl.ds(t * tile, tile)
            head, following = column(0, kk, t), column(1, kk, t)
            for zi, value in ((0, head), (depth - 1, following)):
                at = where(kk, zi)
                xh_ref[at, cols], xl_ref[at, cols] = split(value)
            for i in range(depth - 2, 0, -1):
                at = where(kk, i)
                free = a_ref[at, cols] - cell_ref[1, at, cols] * head
                following = free - cell_ref[0, at, cols] * (link(1, i) * following)
                xh_ref[at, cols], xl_ref[at, cols] = split(following)

    for kk in range(owned):
        substitute(kk)

    def send(m, h):
        lanes = pl.ds((m * halfs + h) * LANES, LANES)
        sent = swap_groups(
            [jnp.concatenate([a_ref[where(kk, zi), lanes] for kk in range(owned)], 0) for zi in range(depth)], group
        )
        for g, block in enumerate(sent):
            for kk in range(owned):
                out_ref[slot(kk, m, g, h), :] = block[kk * blocks : kk * blocks + blocks]

    for m in range(parts):
        at = pl.ds(m * halfs * LANES, halfs * LANES)
        a_ref[:, at] = dot3((xh_ref[...], xl_ref[...]), (sh_ref[:, at], sl_ref[:, at]), ((1,), (0,)))
        for h in range(halfs):
            send(m, h)


WHOLE = pl.BlockSpec(memory_space=VMEM)
PART = 256


def on_chip(*arrays):
    return [pltpu.with_memory_space_constraint(a, VMEM) for a in arrays]


def in_hbm(*arrays):
    return [pltpu.with_memory_space_constraint(a, pltpu.MemorySpace.HBM) for a in arrays]


HBM = pl.BlockSpec(memory_space=pltpu.MemorySpace.HBM)


def call_forward(source, high, low, owned, group):
    depth, rows, width = source.shape
    return pl.pallas_call(
        functools.partial(forward_x, owned=owned, group=group),
        name="forward_x",
        out_shape=jax.ShapeDtypeStruct((width * depth * rows // LANES, LANES), jnp.float32),
        in_specs=[HBM] * 3,
        out_specs=HBM,
        scratch_shapes=[
            pltpu.VMEM(source.shape, jnp.float32),
            pltpu.VMEM((2, depth * rows, width // 2), jnp.bfloat16),
            pltpu.VMEM((2, depth * rows, width // 2), jnp.bfloat16),
            pltpu.VMEM((width, depth * rows), jnp.float32),
            pltpu.VMEM((width * depth * rows // LANES, LANES), jnp.float32),
            pltpu.VMEM(high.shape, jnp.bfloat16),
            pltpu.VMEM(low.shape, jnp.bfloat16),
            pltpu.SemaphoreType.DMA((rows // group + 4,)),
        ],
    )(*in_hbm(source, high, low))


def call_backward(message, high, low, shape, owned, group):
    depth, rows, width = shape
    return pl.pallas_call(
        functools.partial(backward_x, owned=owned, group=group),
        name="backward_x",
        out_shape=jax.ShapeDtypeStruct(shape, jnp.float32),
        in_specs=[WHOLE] * 3,
        out_specs=HBM,
        scratch_shapes=[
            pltpu.VMEM((width, depth * rows), jnp.float32),
            pltpu.VMEM((2, depth * rows, width // 2), jnp.float32),
            pltpu.VMEM(shape, jnp.float32),
            pltpu.SemaphoreType.DMA((rows // group,)),
        ],
        compiler_params=pltpu.CompilerParams(vmem_limit_bytes=40 * 2**20),
    )(*on_chip(message, high, low))


def sine_tables(peers, parts, group):
    width = peers * parts * group
    return pl.pallas_call(
        sine_table,
        name="sine_table",
        out_shape=[pltpu.VMEM((width, width), jnp.bfloat16)] * 2,
        in_specs=[WHOLE] * 4,
        out_specs=[WHOLE] * 2,
    )(*sine_parts(peers, parts, group))


def call_coefficients(widths, eigen_x, eigen_y, depth):
    blocks, owned, wide = widths.shape[0], eigen_x.shape[0], eigen_y.shape[1]
    pitch = -(-owned * (wide // LANES) // SUB) * SUB
    shapes = ((2, owned * depth * blocks, wide), (2, depth * blocks, LANES), (6, blocks * pitch, LANES))
    return pl.pallas_call(
        functools.partial(coefficients, depth=depth, tile=wide // 2),
        name="coefficients",
        out_shape=[jax.ShapeDtypeStruct(s, jnp.float32) for s in shapes],
        in_specs=[WHOLE] * 3,
        out_specs=[WHOLE] * 3,
        scratch_shapes=[
            pltpu.VMEM((blocks + 2 * SUB, LANES), jnp.float32),
            pltpu.VMEM((4, blocks * pitch, LANES), jnp.float32),
        ],
    )(widths, eigen_x, eigen_y)


def call_middle(message, high, low, cell, link, block, *, peers, blocks, depth, parts, group, owned):
    wide = high.shape[1]
    size = (owned * depth * blocks, wide)
    return pl.pallas_call(
        functools.partial(
            middle, peers=peers, blocks=blocks, depth=depth, parts=parts, group=group, owned=owned, tile=wide // 3
        ),
        name="middle",
        out_shape=pltpu.VMEM(message.shape, jnp.float32),
        in_specs=[WHOLE] * 3 + [HBM] * 3,
        out_specs=WHOLE,
        scratch_shapes=[
            pltpu.VMEM(size, jnp.float32),
            pltpu.VMEM(size, jnp.bfloat16),
            pltpu.VMEM(size, jnp.bfloat16),
            pltpu.VMEM((2, *block.shape[1:]), jnp.float32),
            pltpu.VMEM(cell.shape, jnp.float32),
            pltpu.VMEM(link.shape, jnp.float32),
            pltpu.VMEM(block.shape, jnp.float32),
            pltpu.SemaphoreType.DMA((3,)),
        ],
        compiler_params=pltpu.CompilerParams(vmem_limit_bytes=40 * 2**20),
    )(*on_chip(message, high, low), *in_hbm(cell, link, block))


def exchange(rows, devices):
    flat = rows.reshape(devices, 1, -1)
    return lax.all_to_all(flat, ALL, split_axis=0, concat_axis=0, tiled=True).reshape(-1, LANES)


def all_widths(cell_width, blocks):
    depth = cell_width.shape[0]
    row = lax.broadcasted_iota(jnp.int32, (blocks, LANES), 0)
    held = jnp.where(row == lax.axis_index("gz"), jnp.pad(cell_width, (0, LANES - depth))[None], 0.0)
    step = 1
    while step < blocks:
        held = held + lax.ppermute(held, "gz", [(i, i ^ step) for i in range(blocks)])
        step *= 2
    return held


def on_device(source, cell_width):
    depth, rows, width_x = source.shape
    peers, blocks = lax.axis_size("pa"), lax.axis_size("gz")
    devices = peers * blocks
    width_y = rows * peers
    owned = width_x // devices
    group = LANES // depth
    parts = rows // group

    cosines = halves(cosine_rows(width_x)[:, : width_x // 2].reshape(-1, 2, width_x // 2).swapaxes(0, 1).reshape(width_x, -1))
    order = order_y(np.arange(width_y), peers, parts, group)
    sines = sine_tables(peers, parts, group)
    got = exchange(call_forward(source, *cosines, owned, group), devices)

    device, half = lax.axis_index(ALL), devices // 2
    own_k = 2 * (jnp.arange(owned, dtype=jnp.int32) * half + device % half) + device // half
    eigen_x, eigen_y = eigen_first(own_k, width_x)[:, None], eigen_second(jnp.asarray(order), width_y)[None]
    solve = call_coefficients(all_widths(cell_width, blocks), eigen_x, eigen_y, depth)
    back = call_middle(
        got, *sines, *solve,
        peers=peers, blocks=blocks, depth=depth, parts=parts, group=group, owned=owned,
    )
    return call_backward(exchange(back, devices), *cosines, source.shape, owned, group)


def solution(mesh):
    return jax.shard_map(
        on_device,
        mesh=mesh,
        in_specs=(P("gz", "pa", None), P("gz")),
        out_specs=P("gz", "pa", None),
        check_vma=False,
    )
```
